32 devices in a mesh: data: 2 (over x), seq: 4 (over z), branch: 4 (over y, core).
Axes of the slice: x: 2, y: 2, z: 4, core: 2. Of those that a mesh axis runs over, the one named last changes fastest.
Arguments:
- latents: bfloat16 [2, 1024, 2432], P('data', ('seq', 'branch')), parts along dimension 0
- hint_emb: bfloat16 [2, 1024, 2432], P('data', ('seq', 'branch')), parts along dimension 0
- in_qkv: bfloat16 [2, 3, 2432, 7296], replicated
- in_proj: bfloat16 [2, 3, 38, 64, 2432], replicated
- in_up: bfloat16 [2, 3, 2432, 9728], replicated
- in_down: bfloat16 [2, 3, 9728, 2432], replicated
- out_qkv: bfloat16 [2, 2432, 7296], replicated
- out_proj: bfloat16 [2, 38, 64, 2432], replicated
- out_up: bfloat16 [2, 2432, 9728], replicated
- out_down: bfloat16 [2, 9728, 2432], replicated
- hint_proj: bfloat16 [2432, 2432], replicated
- zero_proj: bfloat16 [3, 2432, 2432], replicated
- skip_proj: bfloat16 [2, 4864, 2432], replicated
- final_proj: bfloat16 [2432, 2432], replicated
Outputs:
- output: bfloat16 [2, 1024, 2432], P('data', ('seq', 'branch')), parts along dimension 0
There are 2 independent parts. The reference program is written for one: setup_inputs(seed, part) draws one part's arguments, and reference() takes and returns one part's arrays. A program takes and returns all parts, laid end to end along the dimension named above; an argument that names none is the same for every part.
All inputs are finite; a program needn't handle non-finite values.
Results may differ from the reference program's by a relative error of at most 0.02.
Values are sent between devices in bfloat16 or wider.
A program may use at most 4.75 GiB of HBM per device.

```python
import math
import jax
import jax.numpy as jnp
from jax import lax

D = 2432
HEADS = 38
IN_BLOCKS = 2
TOKENS = 1024
HEAD = D // HEADS
EPS = 1e-6


def draw_normal(key, shape, scale):
    return (jax.random.normal(key, shape, jnp.float32) * scale).astype(jnp.bfloat16)


def setup_inputs(seed: int = 0, part: int = 0) -> dict:
    data_key = jax.random.fold_in(jax.random.key(seed), part)
    key_lat, key_hint = jax.random.split(data_key)
    weight_keys = jax.random.split(jax.random.key(seed + 1), 12)
    inv_root = D ** -0.5
    sharpness = math.sqrt(max(math.log(TOKENS / 16.0), 1.0))
    qkv_scale = jnp.concatenate([jnp.full((D,), sharpness * inv_root), jnp.full((2 * D,), inv_root)])
    skip_scale = jnp.concatenate([jnp.full((D, 1), inv_root), jnp.full((D, 1), 0.6 * inv_root)])
    down_scale = (4 * D) ** -0.5
    return {
        'latents': draw_normal(key_lat, (1, TOKENS, D), 1.0),
        'hint_emb': draw_normal(key_hint, (1, TOKENS, D), 1.0),
        'in_qkv': draw_normal(weight_keys[0], (2, IN_BLOCKS + 1, D, 3 * D), qkv_scale),
        'in_proj': draw_normal(weight_keys[1], (2, IN_BLOCKS + 1, HEADS, HEAD, D), 2.0 * inv_root),
        'in_up': draw_normal(weight_keys[2], (2, IN_BLOCKS + 1, D, 4 * D), inv_root),
        'in_down': draw_normal(weight_keys[3], (2, IN_BLOCKS + 1, 4 * D, D), down_scale),
        'out_qkv': draw_normal(weight_keys[4], (IN_BLOCKS, D, 3 * D), qkv_scale),
        'out_proj': draw_normal(weight_keys[5], (IN_BLOCKS, HEADS, HEAD, D), 2.0 * inv_root),
        'out_up': draw_normal(weight_keys[6], (IN_BLOCKS, D, 4 * D), inv_root),
        'out_down': draw_normal(weight_keys[7], (IN_BLOCKS, 4 * D, D), down_scale),
        'hint_proj': draw_normal(weight_keys[8], (D, D), inv_root),
        'zero_proj': draw_normal(weight_keys[9], (IN_BLOCKS + 1, D, D), 0.6 * inv_root),
        'skip_proj': draw_normal(weight_keys[10], (IN_BLOCKS, 2 * D, D), skip_scale),
        'final_proj': draw_normal(weight_keys[11], (D, D), inv_root),
    }


def layer_norm(values):
    values = values.astype(jnp.float32)
    mean_val = jnp.mean(values, axis=-1, keepdims=True)
    centered = values - mean_val
    var_val = jnp.mean(centered * centered, axis=-1, keepdims=True)
    return (centered * lax.rsqrt(var_val + EPS)).astype(jnp.bfloat16)


def matmul(left_op, right_op):
    return jnp.dot(left_op, right_op, preferred_element_type=jnp.float32).astype(jnp.bfloat16)


def add_bf16(left_op, right_op):
    return (left_op.astype(jnp.float32) + right_op.astype(jnp.float32)).astype(jnp.bfloat16)


def attention(normed, w_qkv):
    qkv_rows = matmul(normed, w_qkv)
    q_heads = qkv_rows[:, :D].reshape(TOKENS, HEADS, HEAD).transpose(1, 0, 2)
    k_heads = qkv_rows[:, D:2 * D].reshape(TOKENS, HEADS, HEAD).transpose(1, 0, 2)
    v_heads = qkv_rows[:, 2 * D:].reshape(TOKENS, HEADS, HEAD).transpose(1, 0, 2)

    def one_head(operands):
        q_one, k_one, v_one = operands
        scores = jnp.dot(q_one, k_one.T, preferred_element_type=jnp.float32) * (HEAD ** -0.5)
        attn_probs = jax.nn.softmax(scores, axis=-1).astype(jnp.bfloat16)
        return jnp.dot(attn_probs, v_one, preferred_element_type=jnp.float32).astype(jnp.bfloat16)

    mixed_rows = lax.map(one_head, (q_heads, k_heads, v_heads))
    return mixed_rows.transpose(1, 0, 2).reshape(TOKENS, D)


def run_block(residual, weights):
    w_qkv, w_proj, w_up, w_down = weights
    mixed_rows = attention(layer_norm(residual), w_qkv)
    residual = add_bf16(residual, matmul(mixed_rows, w_proj.reshape(D, D)))
    hidden = matmul(layer_norm(residual), w_up)
    activated = jax.nn.gelu(hidden.astype(jnp.float32)).astype(jnp.bfloat16)
    return add_bf16(residual, matmul(activated, w_down))


def reference(latents, hint_emb, in_qkv, in_proj, in_up, in_down, out_qkv, out_proj, out_up, out_down, hint_proj, zero_proj, skip_proj, final_proj):
    base_in = latents[0]
    control_in = add_bf16(base_in, matmul(hint_emb[0], hint_proj))

    def base_step(residual, weights):
        residual = run_block(residual, weights)
        return residual, residual

    def control_step(residual, weights):
        w_qkv, w_proj, w_up, w_down, w_zero = weights
        residual = run_block(residual, (w_qkv, w_proj, w_up, w_down))
        return residual, matmul(residual, w_zero)

    def out_step(residual, weights):
        w_qkv, w_proj, w_up, w_down, w_skip, skip_rows = weights
        merged = matmul(jnp.concatenate([residual, skip_rows], axis=-1), w_skip)
        return run_block(merged, (w_qkv, w_proj, w_up, w_down)), None

    base_last, base_stack = lax.scan(base_step, base_in, (in_qkv[0], in_proj[0], in_up[0], in_down[0]))
    control_last, control_stack = lax.scan(control_step, control_in, (in_qkv[1], in_proj[1], in_up[1], in_down[1], zero_proj))
    skip_sums = add_bf16(base_stack, control_stack)
    out_weights = (out_qkv, out_proj, out_up, out_down, skip_proj, skip_sums[:IN_BLOCKS][::-1])
    final_res, unused_ys = lax.scan(out_step, skip_sums[IN_BLOCKS], out_weights)
    return matmul(layer_norm(final_res), final_proj)[None]
```

```python
import functools
import jax
import jax.numpy as jnp
from jax import lax
from jax.experimental import pallas as pl
from jax.experimental.pallas import tpu as pltpu
from jax.sharding import PartitionSpec as P

EPS = 1e-6
D = 2432
HALF_UP = 4864
LANES = 128
TOK = 1024
SLOTS = 60
MESH_ID = pl.DeviceIdType.MESH
BF16 = jnp.bfloat16
F32 = jnp.float32


def aligned(value, unit):
    return value if isinstance(value, int) else pl.multiple_of(value, unit)


class WeightRing:
    def __init__(self, segments, buf, sem):
        self.buf, self.sem = buf, sem
        self.bounds = []
        first = 0
        for count, source in segments:
            self.bounds.append((first, first + count, source))
            first += count
        self.total = first
        self.any_source = segments[0][1](0)

    def start(self, base, off, span):
        unit = base + off
        for first, last, source in self.bounds:
            lo, hi = max(first, base), min(last, base + span)
            if lo >= hi or isinstance(unit, int) and not first <= unit < last:
                continue

            def issue(first=first, source=source):
                slot = lax.rem(jnp.int32(unit), SLOTS)
                pltpu.make_async_copy(source(unit - first), self.buf.at[slot], self.sem.at[slot]).start()

            if isinstance(unit, int) or lo == base and hi == base + span:
                issue()
            else:
                pl.when(jnp.logical_and(unit >= first, unit < last))(issue)

    def fill(self):
        for first, last, source in self.bounds:
            last = min(last, SLOTS)
            if first >= last:
                break

            @pl.loop(first, last)
            def _(unit, first=first, source=source):
                pltpu.make_async_copy(source(unit - first), self.buf.at[unit], self.sem.at[unit]).start()

    def wait(self, unit):
        slot = lax.rem(jnp.int32(unit), SLOTS)
        pltpu.make_async_copy(self.any_source, self.buf.at[slot], self.sem.at[slot]).wait()
        return slot

    def load(self, units):
        slots = [self.wait(unit) for unit in units]
        parts = [self.buf[slot] for slot in slots]
        return parts[0] if len(parts) == 1 else jnp.concatenate(parts, axis=1)


def matmul(lhs, rhs):
    return jnp.dot(lhs, rhs, preferred_element_type=F32)


def add_f32(left, right):
    return left.astype(F32) + right.astype(F32)


def ln_rows(src, dst, rows):
    for r0 in range(0, rows, 32):
        val = src[r0:r0 + 32, :].astype(F32)
        cen = val - jnp.mean(val, axis=-1, keepdims=True)
        var = jnp.mean(cen * cen, axis=-1, keepdims=True)
        dst[r0:r0 + 32, :] = (cen * lax.rsqrt(var + EPS)).astype(BF16)


def step_kernel(num_in, lat, hint, in_qkv, in_proj, in_up, in_down, out_qkv, out_proj, out_up, out_down, hint_w, zero_w, skip_w, final_w, y_ref,
                wbuf, xl, hi, msg, u, x, act, po, ps, pin, qin, stg, o_st, a_in, vv, part, rx, skp,
                wsem, init_sem, xs_sem, xr_sem, us_sem, ur_sem, qs_sem, qr_sem, as_sem, ar_sem, ps_sem, pr_sem, es_sem, er_sem):
    data_id = lax.axis_index('data')
    seq_id = lax.axis_index('seq')
    branch_id = lax.axis_index('branch')
    core = branch_id % 2
    row_y = branch_id // 2
    side = seq_id // 2
    quad = 2 * row_y + seq_id % 2
    chip = 4 * side + quad

    def device(side_id, quad_id, core_id):
        return (data_id, 2 * side_id + quad_id % 2, 2 * (quad_id // 2) + core_id)

    peer = device(side, quad, 1 - core)
    partner = device(1 - side, quad, core)

    def remote(src, dst, send, recv, dev):
        return pltpu.make_async_remote_copy(src_ref=src, dst_ref=dst, send_sem=send, recv_sem=recv, device_id=dev, device_id_type=MESH_ID)

    def layout(is_in):
        n_chips = 4 if is_in else 8
        me = quad if is_in else chip
        bits = 2 if is_in else 3

        def extra_dest(idx):
            return 2 * idx + core if is_in else 1 + 5 * idx + 3 * core

        def combo(j):
            extra = j // 8
            rel = (n_chips - 1) - j % n_chips
            prim = 0
            for bit in range(bits):
                step = 2 ** bit
                prim = prim + step * ((me // step + rel // step) % 2)
            slot_p = j // n_chips
            num_p = 10 * core + slot_p * n_chips + prim
            num_x = 10 * core + j
            num_x = num_x - num_x // 19
            dest = (1 - extra) * prim + extra * extra_dest(j - 8)
            slot = (1 - extra) * slot_p + extra * (8 // n_chips)
            num = (1 - extra) * num_p + extra * num_x
            return dest, slot, num, j + core < 10

        def owner(num):
            plane, j = num // 10, num % 10
            if j < 8:
                return plane, j % n_chips
            return plane, (2 * (j - 8) + plane if is_in else 1 + 5 * (j - 8) + 3 * plane)

        return n_chips, me, combo, owner, extra_dest

    def chip_device(is_in, idx, core_id):
        return device(side, idx, core_id) if is_in else device(idx // 4, idx % 4, core_id)

    def cols(start):
        return pl.ds(aligned(start, LANES), LANES)

    def square(ref, *lead):
        return (19, lambda j: ref.at[(*lead, slice(None), cols(j * LANES))])

    def qkv_segment(is_in, *lead):
        ref = in_qkv if is_in else out_qkv
        combo = layout(is_in)[2]
        return (30, lambda j: ref.at[(*lead, slice(None), cols((j % 3) * D + combo(j // 3)[2] * LANES))])

    def up_segment(ref, *lead):
        return (38, lambda j: ref.at[(*lead, slice(None), cols(core * HALF_UP + j * LANES))])

    def down_segment(ref, *lead):
        def source(j):
            last, tile, r = j // 36, j // 4, j % 4
            k_sub = (1 - last) * (r // 2) + last * r
            col = 2 * tile + (1 - last) * (r % 2)
            return ref.at[(*lead, pl.ds(aligned(core * HALF_UP + k_sub * D, LANES), D), cols(col * LANES))]
        return (38, source)

    def skip_segment(idx, half):
        return (19, lambda j: skip_w.at[idx, pl.ds(half * D, D), cols(j * LANES)])

    num_out = num_in
    segments = []
    marks = {}

    def put(name, segment):
        marks[name] = sum(seg[0] for seg in segments)
        segments.append(segment)

    put('hint', square(hint_w))
    for blk in range(num_in + 1):
        put(('qkv', 1, blk), qkv_segment(True, side, blk))
        if blk > 0:
            put(('zero', blk - 1), square(zero_w, blk - 1))
        put(('proj', 1, blk), square(in_proj, side, blk))
        put(('up', 1, blk), up_segment(in_up, side, blk))
        put(('down', 1, blk), down_segment(in_down, side, blk))
    put(('zero', num_in), square(zero_w, num_in))
    put(('skip_s', 0), skip_segment(0, 1))
    put(('skip_o', 0), skip_segment(0, 0))
    for blk in range(num_out):
        put(('qkv', 0, blk), qkv_segment(False, blk))
        if blk + 1 < num_out:
            put(('skip_s', blk + 1), skip_segment(blk + 1, 1))
        put(('proj', 0, blk), square(out_proj, blk))
        put(('up', 0, blk), up_segment(out_up, blk))
        put(('down', 0, blk), down_segment(out_down, blk))
        if blk + 1 < num_out:
            put(('skip_o', blk + 1), skip_segment(blk + 1, 0))
    put('final', square(final_w))
    ring = WeightRing(segments, wbuf, wsem)

    def mm(name, units, lhs, emit, k_subs=1):
        first = marks[name]
        per = 2 * k_subs

        def tile(t, width):
            base = t * per
            acc = None
            for k in range(k_subs):
                rhs = ring.load([first + base + k * width + i for i in range(width)])
                term = matmul(lhs(k), rhs)
                acc = term if acc is None else acc + term
            emit(aligned(t * 256, 256), width * LANES, acc)
            for r in range(width * k_subs):
                ring.start(first + SLOTS, base + r, units)

        pl.loop(0, units // per)(lambda t: tile(t, 2))
        if units % per:
            tile(units // per, 1)

    get_lat = pltpu.make_async_copy(lat.at[0], xl, init_sem.at[0])
    get_hint = pltpu.make_async_copy(hint.at[0], hi, init_sem.at[1])
    get_hint.start()
    get_lat.start()
    ring.fill()
    barrier = pltpu.get_barrier_semaphore()
    my_index = seq_id * 4 + branch_id
    for k in range(1, 16):
        other = (my_index + k) % 16
        pl.semaphore_signal(barrier, inc=1, device_id=(data_id, other // 4, other % 4), device_id_type=MESH_ID)
    pl.semaphore_wait(barrier, 15)
    get_lat.wait()
    get_hint.wait()

    mine = pl.ds(pl.multiple_of(side * 64, 64), 64)
    theirs = pl.ds(pl.multiple_of((1 - side) * 64, 64), 64)

    def emit_hint(col, width, acc):
        base_in = xl[:, pl.ds(col, width)]
        control_in = add_f32(base_in, acc.astype(BF16)).astype(BF16)
        is_base = side == 0
        u[mine, pl.ds(col, width)] = jnp.where(is_base, base_in, control_in)
        msg[:, pl.ds(col, width)] = jnp.where(is_base, control_in, base_in)

    mm('hint', 19, lambda k: hi[...], emit_hint)
    swap = remote(msg, u.at[mine], us_sem, ur_sem, partner)
    swap.start()
    swap.wait()

    def exchange_rows(rows):
        ln_rows(u, x, rows)
        send = remote(x.at[pl.ds(0, rows)], x.at[pl.ds(rows, rows)], xs_sem, xr_sem, peer)
        send.start()
        send.wait_recv()
        return send

    def run_block(is_in, blk, fill_in, before_proj):
        rows = 128 if is_in else 64
        chip_rows = 2 * rows
        n_chips, me, combo, owner, extra_dest = layout(is_in)
        key = (1 if is_in else 0, blk)
        extra_slot = 8 // n_chips

        sent = exchange_rows(rows)

        def piece_copy(j, dest, slot):
            return remote(stg.at[j, pl.ds(0, chip_rows)], qin.at[slot, pl.ds(pl.multiple_of(me * chip_rows, chip_rows), chip_rows)],
                          qs_sem.at[j], qr_sem.at[slot, me], chip_device(is_in, dest, core))

        first = marks[('qkv',) + key]

        @pl.loop(0, 10)
        def _(j):
            dest, slot, num, valid = combo(j)
            rhs = ring.load([first + 3 * j + i for i in range(3)])

            @pl.when(valid)
            def _():
                stg[j, 0:chip_rows, :] = matmul(x[0:chip_rows, :], rhs).astype(BF16)

                @pl.when(dest != me)
                def _():
                    piece_copy(j, dest, slot).start()

                @pl.when(dest == me)
                def _():
                    qin[slot, pl.ds(pl.multiple_of(me * chip_rows, chip_rows), chip_rows), :] = stg[j, 0:chip_rows, :]

            for i in range(3):
                ring.start(first + SLOTS, 3 * j + i, 30)

        sent.wait_send()
        fill_in()

        def send_copies(slot, num):
            copies = []
            col = cols(num * LANES)
            for k in range(n_chips):
                idx = (me + k) % n_chips
                for which in range(2):
                    if k == 0 and which == 0:
                        continue
                    to_core = core if which == 0 else 1 - core
                    src = o_st.at[slot, pl.ds(pl.multiple_of(idx * chip_rows + which * rows, rows), rows)]
                    copies.append(remote(src, a_in.at[pl.ds(0, rows), col], as_sem.at[slot, 2 * k + which], ar_sem.at[num], chip_device(is_in, idx, to_core)))
            return copies

        def attend(slot, num):
            for k in range(1, n_chips):
                src = (me + k) % n_chips
                remote(stg.at[0, pl.ds(0, chip_rows)], qin.at[slot, pl.ds(pl.multiple_of(src * chip_rows, chip_rows), chip_rows)],
                       qs_sem.at[0], qr_sem.at[slot, src], peer).wait_recv()
            low = lax.broadcasted_iota(jnp.int32, (TOK, LANES), 1) < 64
            v_pair = qin[slot, :, 2 * LANES:3 * LANES]
            zero = jnp.zeros_like(v_pair)
            vv[0:TOK, :] = jnp.where(low, v_pair, zero)
            vv[TOK:2 * TOK, :] = jnp.where(low, zero, v_pair)

            @pl.loop(0, TOK // 128)
            def _(i):
                q_rows = pl.ds(pl.multiple_of(i * 128, 128), 128)
                q_pair = (qin[slot, q_rows, 0:LANES].astype(F32) * 0.125).astype(BF16)
                low_q = lax.broadcasted_iota(jnp.int32, (128, LANES), 1) < 64
                none = jnp.zeros_like(q_pair)
                q_both = jnp.concatenate([jnp.where(low_q, q_pair, none), jnp.where(low_q, none, q_pair)], axis=0)
                scores = lax.dot_general(q_both, qin[slot, :, LANES:2 * LANES], (((1,), (1,)), ((), ())), preferred_element_type=F32)
                weights = jnp.exp(scores - jnp.max(scores, axis=-1, keepdims=True))
                inv = 1.0 / jnp.sum(weights, axis=-1, keepdims=True)
                probs = weights.astype(BF16)
                mixed = matmul(jnp.concatenate([probs[0:128], probs[128:256]], axis=1), vv[...])
                o_st[slot, q_rows, :] = (mixed * jnp.where(low_q, inv[0:128], inv[128:256])).astype(BF16)

            a_in[0:rows, cols(num * LANES)] = o_st[slot, pl.ds(pl.multiple_of(me * chip_rows, chip_rows), rows), :]
            for copy in send_copies(slot, num):
                copy.start()

        for slot in range(extra_slot):
            attend(slot, 10 * core + slot * n_chips + me)
        holds_first = extra_dest(0) == me
        holds_second = jnp.logical_and(extra_dest(1) == me, core == 0)
        extra_num = 10 * core + 8 + holds_second.astype(jnp.int32)
        holds_extra = jnp.logical_or(holds_first, holds_second)

        @pl.when(holds_extra)
        def _():
            attend(extra_slot, extra_num)

        @pl.loop(0, 10)
        def _(j):
            dest, slot, num, valid = combo(j)

            @pl.when(jnp.logical_and(valid, dest != me))
            def _():
                piece_copy(j, dest, slot).wait_send()

        for num in range(19):
            plane, dest = owner(num)

            @pl.when(jnp.logical_not(jnp.logical_and(core == plane, me == dest)))
            def _(num=num):
                remote(o_st.at[0, pl.ds(0, rows)], a_in.at[pl.ds(0, rows), num * LANES:(num + 1) * LANES], as_sem.at[0, 0], ar_sem.at[num], peer).wait_recv()

        before_proj()

        def emit_proj(col, width, acc):
            u[0:rows, pl.ds(col, width)] = add_f32(u[0:rows, pl.ds(col, width)], acc.astype(BF16)).astype(BF16)

        mm(('proj',) + key, 19, lambda k: a_in[0:rows, :], emit_proj)

        for slot in range(extra_slot):
            for copy in send_copies(slot, 10 * core + slot * n_chips + me):
                copy.wait_send()

        @pl.when(holds_extra)
        def _():
            for copy in send_copies(extra_slot, extra_num):
                copy.wait_send()

        sent = exchange_rows(rows)

        def emit_up(col, width, acc):
            hidden = acc.astype(BF16).astype(F32)
            act[0:chip_rows, pl.ds(col, width)] = jax.nn.gelu(hidden).astype(BF16)

        mm(('up',) + key, 38, lambda k: x[0:chip_rows, :], emit_up)

        def partial_copy(col, width):
            tile = col // 256
            return remote(ps.at[pl.ds(0, rows), pl.ds(col, width)], pin.at[pl.ds(0, rows), pl.ds(col, width)], ps_sem.at[tile], pr_sem.at[tile], peer)

        def emit_down(col, width, acc):
            po[0:rows, pl.ds(col, width)] = acc[0:rows]
            ps[0:rows, pl.ds(col, width)] = acc[rows:chip_rows]
            partial_copy(col, width).start()

        sent.wait_send()
        mm(('down',) + key, 38, lambda k: act[0:chip_rows, k * D:(k + 1) * D], emit_down, k_subs=2)

        def finish(col, width):
            partial_copy(col, width).wait()
            total = (po[0:rows, pl.ds(col, width)] + pin[0:rows, pl.ds(col, width)]).astype(BF16)
            u[0:rows, pl.ds(col, width)] = add_f32(u[0:rows, pl.ds(col, width)], total).astype(BF16)

        pl.loop(0, 9)(lambda t: finish(aligned(t * 256, 256), 256))
        finish(9 * 256, LANES)

    def make_part(idx):
        def emit(col, width, acc):
            part[idx, :, pl.ds(col, width)] = jnp.where(side == 0, u[:, pl.ds(col, width)], acc.astype(BF16))
        mm(('zero', idx), 19, lambda k: u[...], emit)

    def part_copy(idx):
        return remote(part.at[idx, theirs], rx.at[idx], es_sem.at[idx], er_sem.at[idx], partner)

    nothing = lambda: None
    for blk in range(num_in + 1):
        if blk == 0:
            run_block(True, blk, nothing, nothing)
        else:
            run_block(True, blk, functools.partial(make_part, blk - 1), lambda blk=blk: part_copy(blk - 1).start())
    make_part(num_in)
    part_copy(num_in).start()
    for idx in range(num_in):
        part_copy(idx).wait()
        rx[idx] = add_f32(part[idx, mine, :], rx[idx]).astype(BF16)

    def skip_part(blk):
        def emit(col, width, acc):
            skp[:, pl.ds(col, width)] = acc
        mm(('skip_s', blk), 19, lambda k: rx[num_in - 1 - blk], emit)

    def merge(blk):
        def emit(col, width, acc):
            msg[:, pl.ds(col, width)] = (skp[:, pl.ds(col, width)] + acc).astype(BF16)
        mm(('skip_o', blk), 19, lambda k: u[0:64, :], emit)
        u[0:64, :] = msg[...]

    skip_part(0)
    part_copy(num_in).wait()
    u[0:64, :] = add_f32(part[num_in, mine, :], rx[num_in]).astype(BF16)
    for blk in range(num_out):
        merge(blk)
        run_block(False, blk, functools.partial(skip_part, blk + 1) if blk + 1 < num_out else nothing, nothing)

    ln_rows(u, x, 64)

    def emit_final(col, width, acc):
        y_ref[0, :, pl.ds(col, width)] = acc.astype(BF16)

    mm('final', 19, lambda k: x[0:64, :], emit_final)


def solution(mesh):
    row_spec = P('data', ('seq', 'branch'), None)

    def device_fn(latents, hint_emb, in_qkv, in_proj, in_up, in_down, out_qkv, out_proj, out_up, out_down, hint_proj, zero_proj, skip_proj, final_proj):
        num_in = out_qkv.shape[0]
        in_proj = in_proj.reshape(2, num_in + 1, D, D)
        out_proj = out_proj.reshape(num_in, D, D)
        anywhere = pl.BlockSpec(memory_space=pl.ANY)
        dma = pltpu.SemaphoreType.DMA
        return pl.pallas_call(
            functools.partial(step_kernel, num_in),
            out_shape=jax.ShapeDtypeStruct((1, 64, D), BF16),
            in_specs=[anywhere] * 14,
            out_specs=pl.BlockSpec(memory_space=pltpu.VMEM),
            scratch_shapes=[
                pltpu.VMEM((SLOTS, D, LANES), BF16),
                pltpu.VMEM((64, D), BF16),
                pltpu.VMEM((64, D), BF16),
                pltpu.VMEM((64, D), BF16),
                pltpu.VMEM((128, D), BF16),
                pltpu.VMEM((256, D), BF16),
                pltpu.VMEM((256, HALF_UP), BF16),
                pltpu.VMEM((128, D), F32),
                pltpu.VMEM((128, D), F32),
                pltpu.VMEM((128, D), F32),
                pltpu.VMEM((3, TOK, 3 * LANES), BF16),
                pltpu.VMEM((10, 256, 3 * LANES), BF16),
                pltpu.VMEM((3, TOK, LANES), BF16),
                pltpu.VMEM((128, D), BF16),
                pltpu.VMEM((2 * TOK, LANES), BF16),
                pltpu.VMEM((num_in + 1, 128, D), BF16),
                pltpu.VMEM((num_in + 1, 64, D), BF16),
                pltpu.VMEM((64, D), F32),
                dma((SLOTS,)), dma((2,)), dma, dma, dma, dma,
                dma((10,)), dma((3, 8)), dma((3, 16)), dma((19,)),
                dma((10,)), dma((10,)), dma((num_in + 1,)), dma((num_in + 1,)),
            ],
            compiler_params=pltpu.CompilerParams(collective_id=0, has_side_effects=True, vmem_limit_bytes=67043328),
            name='denoiser_step',
        )(latents, hint_emb, in_qkv, in_proj, in_up, in_down, out_qkv, out_proj, out_up, out_down, hint_proj, zero_proj, skip_proj, final_proj)

    return jax.shard_map(device_fn, mesh=mesh, in_specs=(row_spec, row_spec) + (P(),) * 12, out_specs=row_spec, check_vma=False)
```

```python
import functools
import jax
import jax.numpy as jnp
from jax import lax
from jax.experimental import pallas as pl
from jax.experimental.pallas import tpu as pltpu
from jax.sharding import PartitionSpec as P

EPS = 1e-6
D = 2432
HALF_UP = 4864
LANES = 128
TOK = 1024
UNITS = 49
QUERIES = 256
KEYS = 512
MESH_ID = pl.DeviceIdType.MESH
BF16 = jnp.bfloat16
F32 = jnp.float32


def aligned(value, unit):
    return value if isinstance(value, int) else pl.multiple_of(value, unit)


class Chunk:
    def __init__(self, name, parts, room=0):
        self.name, self.parts, self.room = name, parts, room
        self.width = sum(width for width, _ in parts)
        self.blk = self.pos = self.sem = self.trigger = None


class WeightStream:
    def __init__(self, pre, block, post, num_blocks, buf, sem, blank):
        self.buf, self.sem, self.blank, self.num_blocks = buf, sem, blank, num_blocks
        order = []
        sems = {}

        def add(chunks, blk, kind):
            for chunk in chunks:
                item = Chunk(chunk.name, chunk.parts, chunk.room)
                item.blk, item.kind = blk, kind
                item.sem = sems.setdefault(item.name, len(sems))
                order.append(item)

        add(pre, None, 'pre')
        for blk in range(num_blocks):
            add(block, blk, 'block')
        add(post, None, 'post')
        pos = UNITS - sum(chunk.width for chunk in pre)
        holder = [None] * UNITS
        self.first = []
        self.after = {}
        self.places = {}
        for rank, item in enumerate(order):
            if pos + max(item.width, item.room) > UNITS:
                pos = 0
            item.pos, item.rank = pos, rank
            held = [holder[i] for i in range(pos, pos + item.width) if holder[i] is not None]
            holder[pos:pos + item.width] = [item] * item.width
            pos += item.width
            assert self.places.setdefault(item.name, (item.pos, item.width, item.sem)) == (item.pos, item.width, item.sem)
            if not held:
                self.first.append(item)
                continue
            last = max(held, key=lambda other: other.rank)
            self.after.setdefault(last.name, []).append((last.blk, item))
        self.num_sems = len(sems)

    def issue(self, item, blk):
        off = item.pos
        for width, source in item.parts:
            dst = self.buf.at[:, off * LANES:(off + width) * LANES]
            pltpu.make_async_copy(source(blk), dst, self.sem.at[item.sem]).start()
            off += width

    def fill(self, kind):
        for item in self.first:
            if item.kind == kind:
                self.issue(item, item.blk)

    def wait(self, name, trip, width):
        first, _, sem = self.places[(name, 0 if not isinstance(trip, int) else trip)]
        pos = first if isinstance(trip, int) else first + trip * width
        sem = sem if isinstance(trip, int) else sem + trip
        dst = self.buf.at[:, pl.ds(aligned(pos * LANES, LANES), width * LANES)]
        pltpu.make_async_copy(self.blank(width), dst, self.sem.at[sem]).wait()
        return pos

    def row(self, name, trips):
        places = [self.places[(name, trip)] for trip in range(trips)]
        first, width, sem = places[0]
        assert places == [(first + trip * width, width, sem + trip) for trip in range(trips)]

    def used_trip(self, name, trip, trips, blk):
        if isinstance(trip, int):
            self.used((name, trip), blk)
            return
        for k in range(trips):
            if self.after.get((name, k)):
                pl.when(trip == k)(functools.partial(self.used, (name, k), blk))

    def used(self, name, blk):
        todo = self.after.get(name, [])
        if blk is None:
            for _, item in todo:
                self.issue(item, item.blk)
            return
        seen = set()
        for last_blk, item in todo:
            if item.kind == 'post':
                assert last_blk == self.num_blocks - 1
                pl.when(blk == last_blk)(lambda item=item: self.issue(item, None))
                continue
            step = item.blk - last_blk
            if (item.name, step) in seen:
                continue
            seen.add((item.name, step))
            if step == 0:
                self.issue(item, blk)
            else:
                pl.when(blk < self.num_blocks - 1)(lambda item=item: self.issue(item, blk + 1))


def matmul(lhs, rhs):
    return jnp.dot(lhs, rhs, preferred_element_type=F32)


def add_f32(left, right):
    return left.astype(F32) + right.astype(F32)


def ln_rows(src, dst, rows):
    for r0 in range(0, rows, 32):
        val = src[r0:r0 + 32, :].astype(F32)
        cen = val - jnp.mean(val, axis=-1, keepdims=True)
        var = jnp.mean(cen * cen, axis=-1, keepdims=True)
        dst[r0:r0 + 32, :] = (cen * lax.rsqrt(var + EPS)).astype(BF16)


def step_kernel(num_in, lat, hint, in_qkv, in_proj, in_up, in_down, out_qkv, out_proj, out_up, out_down, hint_w, zero_w, skip_w, final_w, y_ref,
                wbuf, xl, hi, msg, u, x, act, po, ps, pin, qin, stg, o_st, a_in, vt, sb, part, rx, skp,
                wsem, init_sem, xs_sem, xr_sem, us_sem, ur_sem, qs_sem, qr_sem, as_sem, ar_sem, ps_sem, pr_sem, es_sem, er_sem):
    data_id = lax.axis_index('data')
    seq_id = lax.axis_index('seq')
    branch_id = lax.axis_index('branch')
    core = branch_id % 2
    row_y = branch_id // 2
    side = seq_id // 2
    quad = 2 * row_y + seq_id % 2
    chip = 4 * side + quad

    def device(side_id, quad_id, core_id):
        return (data_id, 2 * side_id + quad_id % 2, 2 * (quad_id // 2) + core_id)

    peer = device(side, quad, 1 - core)
    partner = device(1 - side, quad, core)

    def remote(src, dst, send, recv, dev):
        return pltpu.make_async_remote_copy(src_ref=src, dst_ref=dst, send_sem=send, recv_sem=recv, device_id=dev, device_id_type=MESH_ID)

    def layout(is_in):
        n_chips = 4 if is_in else 8
        me = quad if is_in else chip
        bits = 2 if is_in else 3

        def extra_dest(idx):
            return 2 * idx + core if is_in else 1 + 5 * idx + 3 * core

        def combo(j):
            trip, odd = j // 2, j % 2
            extra = trip // 4
            half = n_chips // 2
            rel = (half - 1) - trip % half
            top = me // 2
            prim = (top + rel) % 2 if is_in else 2 * ((top // 2 + rel // 2) % 2) + (top + rel) % 2
            prim = 2 * prim + odd
            slot_p = trip // half
            idx = odd - core
            dest = (1 - extra) * prim + extra * extra_dest(idx)
            slot = (1 - extra) * slot_p + extra * (8 // n_chips)
            num = (1 - extra) * (10 * core + slot_p * n_chips + prim) + extra * (10 * core + 8 + idx)
            return dest, slot, num, extra * core * (1 - odd) == 0

        def owner(num):
            plane, j = num // 10, num % 10
            if j < 8:
                return plane, j % n_chips
            return plane, (2 * (j - 8) + plane if is_in else 1 + 5 * (j - 8) + 3 * plane)

        return n_chips, me, combo, owner, extra_dest

    def chip_device(is_in, idx, core_id):
        return device(side, idx, core_id) if is_in else device(idx // 4, idx % 4, core_id)

    num_blocks = num_in + 1
    num_out = num_in

    def cols(start):
        return pl.ds(aligned(start, LANES), LANES)

    def wide(start, width):
        return pl.ds(aligned(start, LANES), width * LANES)

    def square(name, source):
        return [Chunk((name, trip), [(width, lambda blk, trip=trip, width=width: source(blk, wide(8 * trip * LANES, width)))], 16 if trip == 0 else 0)
                for trip, width in enumerate((8, 8, 3))]

    def qkv_chunks(name, combo, source):
        out = []
        for trip in range(5):
            num = combo(2 * trip)[2]
            out.append(Chunk((name, trip), [(2, lambda blk, num=num, part=part: source(blk, wide(part * D + num * LANES, 2))) for part in range(3)], 30 if trip == 0 else 0))
        return out

    UP_TRIPS = (8, 8, 8, 6, 8)
    DOWN_TRIPS = (4, 4, 4, 4, 3)

    def up_chunks(name, source):
        out, first = [], 0
        for trip, width in enumerate(UP_TRIPS):
            out.append(Chunk((name, trip), [(width, lambda blk, first=first, width=width: source(blk, wide(core * HALF_UP + first * LANES, width)))], 24 if trip == 0 else 0))
            first += width
        return out

    def down_chunks(name, source):
        out, first = [], 0
        for trip, width in enumerate(DOWN_TRIPS):
            out.append(Chunk((name, trip), [
                (width, lambda blk, first=first, width=width, k=k: source(blk, pl.ds(aligned(core * HALF_UP + k * D, LANES), D), wide(first * LANES, width)))
                for k in range(2)], 32 if trip == 0 else 0))
            first += width
        return out

    in_combo, out_combo = layout(True)[2], layout(False)[2]
    pre = square('hint', lambda blk, c: hint_w.at[:, c])
    block = (qkv_chunks('in_qkv', in_combo, lambda blk, c: in_qkv.at[side, blk, :, c])
             + square('in_zero', lambda blk, c: zero_w.at[(blk + num_in) % num_blocks, :, c])
             + square('in_proj', lambda blk, c: in_proj.at[side, blk, :, c])
             + up_chunks('in_up', lambda blk, c: in_up.at[side, blk, :, c])
             + down_chunks('in_down', lambda blk, r, c: in_down.at[side, blk, r, c]))

    def skip_square(idx, half):
        return square(('skip', idx, half), lambda blk, c: skip_w.at[idx, pl.ds(half * D, D), c])

    post = square('zero', lambda blk, c: zero_w.at[num_in, :, c]) + skip_square(0, 1) + skip_square(0, 0)
    for idx in range(num_out):
        post += qkv_chunks(('qkv', idx), out_combo, lambda blk, c, idx=idx: out_qkv.at[idx, :, c])
        if idx + 1 < num_out:
            post += skip_square(idx + 1, 1)
        post += square(('proj', idx), lambda blk, c, idx=idx: out_proj.at[idx, :, c])
        post += up_chunks(('up', idx), lambda blk, c, idx=idx: out_up.at[idx, :, c])
        post += down_chunks(('down', idx), lambda blk, r, c, idx=idx: out_down.at[idx, r, c])
        if idx + 1 < num_out:
            post += skip_square(idx + 1, 0)
    post += square('final', lambda blk, c: final_w.at[:, c])
    stream = WeightStream(pre, block, post, num_blocks, wbuf, wsem, lambda width: in_up.at[0, 0, :, 0:width * LANES])

    def columns(pos, width):
        return wbuf[:, pl.ds(aligned(pos * LANES, LANES), width * LANES)]

    def mm(blk, name, looped, widths, lhs, emit, done=None, k_subs=1):
        stream.row(name, looped)

        def trip(t, col, width):
            pos = stream.wait(name, t, width * k_subs)
            for first in range(0, width, 2):
                size = min(2, width - first)
                subs = [columns(pos + k * width + first, size) for k in range(k_subs)]
                rhs = subs[0] if k_subs == 1 else jnp.concatenate(subs, axis=0)
                emit(aligned(col + first * LANES, LANES), size * LANES, matmul(lhs(), rhs))
            if done is not None:
                done(aligned(col, LANES), width * LANES)
            stream.used_trip(name, t, looped, blk)

        pl.loop(0, looped)(lambda t: trip(t, t * (widths[0] * LANES), widths[0]))
        col = looped * widths[0] * LANES
        for t in range(looped, len(widths)):
            trip(t, col, widths[t])
            col += widths[t] * LANES

    def mm_square(blk, name, lhs, emit, done=None):
        mm(blk, name, 2, (8, 8, 3), lhs, emit, done)

    def mm_up(blk, name, lhs, emit):
        mm(blk, name, 3, UP_TRIPS, lhs, emit)

    def mm_down(blk, name, lhs, emit, done):
        mm(blk, name, 4, DOWN_TRIPS, lhs, emit, done, 2)

    def each(widths, fn):
        col = 0
        for width in widths:
            fn(col, width * LANES)
            col += width * LANES

    scope = jax.named_scope
    get_lat = pltpu.make_async_copy(lat.at[0], xl, init_sem.at[0])
    get_hint = pltpu.make_async_copy(hint.at[0], hi, init_sem.at[1])
    with scope('barrier'):
        get_hint.start()
        get_lat.start()
        stream.fill('pre')
        barrier = pltpu.get_barrier_semaphore()
        my_index = seq_id * 4 + branch_id
        for k in range(1, 16):
            other = (my_index + k) % 16
            pl.semaphore_signal(barrier, inc=1, device_id=(data_id, other // 4, other % 4), device_id_type=MESH_ID)
        pl.semaphore_wait(barrier, 15)
        get_lat.wait()
        get_hint.wait()

    mine = pl.ds(pl.multiple_of(side * 64, 64), 64)
    theirs = pl.ds(pl.multiple_of((1 - side) * 64, 64), 64)

    def swap_copy(col, width):
        return remote(msg.at[:, pl.ds(col, width)], u.at[mine, pl.ds(col, width)], us_sem.at[col // 1024], ur_sem.at[col // 1024], partner)

    def emit_hint(col, width, acc):
        base_in = xl[:, pl.ds(col, width)]
        control_in = add_f32(base_in, acc.astype(BF16)).astype(BF16)
        is_base = side == 0
        u[mine, pl.ds(col, width)] = jnp.where(is_base, base_in, control_in)
        msg[:, pl.ds(col, width)] = jnp.where(is_base, control_in, base_in)

    with scope('hint'):
        mm_square(None, 'hint', lambda: hi[...], emit_hint, lambda col, width: swap_copy(col, width).start())
        stream.fill('block')
    with scope('swap'):
        each((8, 8, 3), lambda col, width: swap_copy(col, width).wait())

    def exchange_rows(rows):
        ln_rows(u, x, rows)
        send = remote(x.at[pl.ds(0, rows)], x.at[pl.ds(rows, rows)], xs_sem, xr_sem, peer)
        send.start()
        send.wait_recv()
        return send

    def run_block(is_in, blk, names, bank, fill_in, before_proj):
        rows = 128 if is_in else 64
        chip_rows = 2 * rows
        n_chips, me, combo, owner, extra_dest = layout(is_in)
        extra_slot = 8 // n_chips
        qkv_name, proj_name, up_name, down_name = names

        def chunk(idx, size):
            return pl.ds(aligned(idx * size, size), size)

        with scope('ln1'):
            sent = exchange_rows(rows)

        def piece_copy(j, dest, slot):
            at = 3 * bank + slot
            return remote(stg.at[j, pl.ds(0, chip_rows)], qin.at[at, chunk(me, chip_rows)], qs_sem.at[j], qr_sem.at[at, me], chip_device(is_in, dest, core))

        def qkv_trip(trip):
            pos = stream.wait(qkv_name, trip, 6)
            for part in range(3):
                both = matmul(x[0:chip_rows, :], columns(pos + 2 * part, 2)).astype(BF16)
                stg[2 * trip, 0:chip_rows, part * LANES:(part + 1) * LANES] = both[:, 0:LANES]
                stg[2 * trip + 1, 0:chip_rows, part * LANES:(part + 1) * LANES] = both[:, LANES:2 * LANES]
            for j in (2 * trip, 2 * trip + 1):
                dest, slot, num, valid = combo(j)

                @pl.when(jnp.logical_and(valid, dest != me))
                def _(j=j, dest=dest, slot=slot):
                    piece_copy(j, dest, slot).start()

                @pl.when(jnp.logical_and(valid, dest == me))
                def _(j=j, slot=slot):
                    qin[3 * bank + slot, chunk(me, chip_rows), :] = stg[j, 0:chip_rows, :]

            stream.used_trip(qkv_name, trip, 5, blk)

        with scope('qkv'):
            stream.row(qkv_name, 5)
            pl.loop(0, 5)(qkv_trip)

        sent.wait_send()
        with scope('fill'):
            fill_in()

        holds = [(extra_dest(0) == me).astype(jnp.int32), jnp.logical_and(extra_dest(1) == me, core == 0).astype(jnp.int32)]
        num_slots = extra_slot + holds[0] + holds[1]

        def slot_pair(slot):
            extra = slot // extra_slot
            return (1 - extra) * (10 * core + slot * n_chips + me) + extra * (10 * core + 8 + holds[1])

        per_chunk = QUERIES // chip_rows

        def query_chunk(i):
            return (me // per_chunk + 1 + i) % (TOK // QUERIES)

        def send_copies(slot, i):
            copies = []
            num = slot_pair(slot)
            first = query_chunk(i) * per_chunk
            chips = [(first + n, True) for n in range(per_chunk)]
            if i == TOK // QUERIES - 1:
                chips = [(me, False)] if per_chunk == 1 else [(me + 1 - 2 * (me % 2), True), (me, False)]
            for n, (idx, other) in enumerate(chips):
                for which in range(2):
                    if not other and which == 0:
                        continue
                    to_core = core if which == 0 else 1 - core
                    src = o_st.at[slot, pl.ds(pl.multiple_of(idx * chip_rows + which * rows, rows), rows)]
                    copies.append(remote(src, a_in.at[pl.ds(0, rows), cols(num * LANES)], as_sem.at[slot, 4 * i + 2 * n + which], ar_sem.at[num], chip_device(is_in, idx, to_core)))
            return copies

        def attend(slot):
            at = 3 * bank + slot
            with scope('att_wait'):
                for k in range(1, n_chips):
                    src = (me + k) % n_chips
                    remote(stg.at[0, pl.ds(0, chip_rows)], qin.at[at, chunk(src, chip_rows)], qs_sem.at[0], qr_sem.at[at, src], peer).wait_recv()
            vt[...] = qin[at, :, 2 * LANES:3 * LANES].T
            low = lax.broadcasted_iota(jnp.int32, (QUERIES, LANES), 1) < 64

            def trip(now, after, top):
                top_next = total = out_a = out_b = None
                if after is not None:
                    q_pair = (qin[at, chunk(query_chunk(after), QUERIES), 0:LANES].astype(F32) * 0.125).astype(BF16)
                    none = jnp.zeros_like(q_pair)
                    q_both = jnp.concatenate([jnp.where(low, q_pair, none), jnp.where(low, none, q_pair)], axis=0)
                for k0 in range(0, TOK, KEYS):
                    keys = slice(k0, k0 + KEYS)
                    if after is not None:
                        score = lax.dot_general(qin[at, keys, LANES:2 * LANES], q_both, (((1,), (1,)), ((), ())), preferred_element_type=F32)
                        sb[after % 2, keys, :] = score
                        part_top = jnp.max(score.reshape(KEYS // 8, 8, 2 * QUERIES), axis=0)
                        top_next = part_top if top_next is None else jnp.maximum(top_next, part_top)
                    if now is not None:
                        weight = jnp.exp(sb[now % 2, keys, :] - top)
                        part_sum = jnp.sum(weight.reshape(KEYS // 8, 8, 2 * QUERIES), axis=0)
                        total = part_sum if total is None else total + part_sum
                        prob = weight.astype(BF16)
                        term_a = matmul(vt[0:64, keys], prob[:, 0:QUERIES])
                        term_b = matmul(vt[64:128, keys], prob[:, QUERIES:2 * QUERIES])
                        out_a = term_a if out_a is None else out_a + term_a
                        out_b = term_b if out_b is None else out_b + term_b
                if now is not None:
                    inv = 1.0 / jnp.sum(total, axis=0, keepdims=True)
                    mixed = jnp.concatenate([out_a * inv[:, 0:QUERIES], out_b * inv[:, QUERIES:2 * QUERIES]], axis=0)
                    o_st[slot, chunk(query_chunk(now), QUERIES), :] = mixed.T.astype(BF16)
                    for copy in send_copies(slot, now):
                        copy.start()
                return None if after is None else jnp.max(top_next, axis=0, keepdims=True)

            last = TOK // QUERIES - 1
            top = trip(None, 0, None)
            for i in range(last):
                top = trip(i, i + 1, top)
            trip(last, None, top)
            a_in[0:rows, cols(slot_pair(slot) * LANES)] = o_st[slot, pl.ds(pl.multiple_of(me * chip_rows, chip_rows), rows), :]

        with scope('att'):
            pl.loop(0, num_slots)(attend)

        with scope('await'):
            @pl.loop(0, 10)
            def _(j):
                dest, slot, num, valid = combo(j)

                @pl.when(jnp.logical_and(valid, dest != me))
                def _():
                    piece_copy(j, dest, slot).wait_send()

            for num in range(19):
                plane, dest = owner(num)

                @pl.when(jnp.logical_not(jnp.logical_and(core == plane, me == dest)))
                def _(num=num):
                    remote(o_st.at[0, pl.ds(0, rows)], a_in.at[pl.ds(0, rows), num * LANES:(num + 1) * LANES], as_sem.at[0, 0], ar_sem.at[num], peer).wait_recv()

            before_proj()

        def emit_proj(col, width, acc):
            u[0:rows, pl.ds(col, width)] = add_f32(u[0:rows, pl.ds(col, width)], acc.astype(BF16)).astype(BF16)

        with scope('proj'):
            mm_square(blk, proj_name, lambda: a_in[0:rows, :], emit_proj)

            @pl.loop(0, num_slots)
            def _(slot):
                for i in range(TOK // QUERIES):
                    for copy in send_copies(slot, i):
                        copy.wait_send()

        with scope('ln2'):
            sent = exchange_rows(rows)

        def emit_up(col, width, acc):
            hidden = acc.astype(BF16).astype(F32)
            act[0:chip_rows, pl.ds(col, width)] = jax.nn.gelu(hidden).astype(BF16)

        with scope('up'):
            mm_up(blk, up_name, lambda: x[0:chip_rows, :], emit_up)
            sent.wait_send()

        def partial_copy(col, width):
            tile = col // 512
            return remote(ps.at[pl.ds(0, rows), pl.ds(col, width)], pin.at[pl.ds(0, rows), pl.ds(col, width)], ps_sem.at[tile], pr_sem.at[tile], peer)

        def emit_down(col, width, acc):
            po[0:rows, pl.ds(col, width)] = acc[0:rows]
            ps[0:rows, pl.ds(col, width)] = acc[rows:chip_rows]

        with scope('down'):
            mm_down(blk, down_name, lambda: act[0:chip_rows, :], emit_down, lambda col, width: partial_copy(col, width).start())

        def finish(col, width):
            partial_copy(col, width).wait()
            total = (po[0:rows, pl.ds(col, width)] + pin[0:rows, pl.ds(col, width)]).astype(BF16)
            u[0:rows, pl.ds(col, width)] = add_f32(u[0:rows, pl.ds(col, width)], total).astype(BF16)

        with scope('fin'):
            each(DOWN_TRIPS, finish)

    def make_part(blk, name, idx, after=None):
        def emit(col, width, acc):
            part[idx, :, pl.ds(col, width)] = jnp.where(side == 0, u[:, pl.ds(col, width)], acc.astype(BF16))
        mm_square(blk, name, lambda: u[...], emit, after)

    def part_copy(idx):
        return remote(part.at[idx, theirs], rx.at[idx], es_sem.at[idx], er_sem.at[idx], partner)

    def mid_copy(col, width):
        tile = num_in + col // 1024
        return remote(part.at[num_in, theirs, pl.ds(col, width)], rx.at[num_in, :, pl.ds(col, width)], es_sem.at[tile], er_sem.at[tile], partner)

    nothing = lambda: None

    @pl.loop(0, num_blocks)
    def _(blk):
        def send_part():
            pl.when(blk > 0)(lambda: part_copy(blk - 1).start())

        run_block(True, blk, ('in_qkv', 'in_proj', 'in_up', 'in_down'), blk % 2, lambda: make_part(blk, 'in_zero', (blk + num_in) % num_blocks), send_part)

    with scope('midpart'):
        make_part(None, 'zero', num_in, lambda col, width: mid_copy(col, width).start())
        for idx in range(num_in):
            part_copy(idx).wait()
            rx[idx] = add_f32(part[idx, mine, :], rx[idx]).astype(BF16)

    def skip_part(blk):
        def emit(col, width, acc):
            skp[:, pl.ds(col, width)] = acc
        mm_square(None, ('skip', blk, 1), lambda: rx[num_in - 1 - blk], emit)

    def merge(blk):
        def emit(col, width, acc):
            msg[:, pl.ds(col, width)] = (skp[:, pl.ds(col, width)] + acc).astype(BF16)
        mm_square(None, ('skip', blk, 0), lambda: u[0:64, :], emit)
        u[0:64, :] = msg[...]

    with scope('skip0'):
        skip_part(0)

    def mid_sum(col, width):
        mid_copy(col, width).wait()
        u[0:64, pl.ds(col, width)] = add_f32(part[num_in, mine, pl.ds(col, width)], rx[num_in, :, pl.ds(col, width)]).astype(BF16)

    with scope('midwait'):
        each((8, 8, 3), mid_sum)
    for blk in range(num_out):
        with scope('merge'):
            merge(blk)
        run_block(False, None, (('qkv', blk), ('proj', blk), ('up', blk), ('down', blk)), (num_blocks + blk) % 2, functools.partial(skip_part, blk + 1) if blk + 1 < num_out else nothing, nothing)

    def emit_final(col, width, acc):
        y_ref[0, :, pl.ds(col, width)] = acc.astype(BF16)

    with scope('final'):
        ln_rows(u, x, 64)
        mm_square(None, 'final', lambda: x[0:64, :], emit_final)


def solution(mesh):
    row_spec = P('data', ('seq', 'branch'), None)

    def device_fn(latents, hint_emb, in_qkv, in_proj, in_up, in_down, out_qkv, out_proj, out_up, out_down, hint_proj, zero_proj, skip_proj, final_proj):
        num_in = out_qkv.shape[0]
        in_proj = in_proj.reshape(2, num_in + 1, D, D)
        out_proj = out_proj.reshape(num_in, D, D)
        anywhere = pl.BlockSpec(memory_space=pl.ANY)
        dma = pltpu.SemaphoreType.DMA
        return pl.pallas_call(
            functools.partial(step_kernel, num_in),
            out_shape=jax.ShapeDtypeStruct((1, 64, D), BF16),
            in_specs=[anywhere] * 14,
            out_specs=pl.BlockSpec(memory_space=pltpu.VMEM),
            scratch_shapes=[
                pltpu.VMEM((D, UNITS * LANES), BF16),
                pltpu.VMEM((64, D), BF16),
                pltpu.VMEM((64, D), BF16),
                pltpu.VMEM((64, D), BF16),
                pltpu.VMEM((128, D), BF16),
                pltpu.VMEM((256, D), BF16),
                pltpu.VMEM((256, HALF_UP), BF16),
                pltpu.VMEM((128, D), F32),
                pltpu.VMEM((128, D), F32),
                pltpu.VMEM((128, D), F32),
                pltpu.VMEM((6, TOK, 3 * LANES), BF16),
                pltpu.VMEM((10, 256, 3 * LANES), BF16),
                pltpu.VMEM((3, TOK, LANES), BF16),
                pltpu.VMEM((128, D), BF16),
                pltpu.VMEM((LANES, TOK), BF16),
                pltpu.VMEM((2, TOK, 2 * QUERIES), F32),
                pltpu.VMEM((num_in + 1, 128, D), BF16),
                pltpu.VMEM((num_in + 1, 64, D), BF16),
                pltpu.VMEM((64, D), F32),
                dma((100,)), dma((2,)), dma, dma, dma((10,)), dma((10,)),
                dma((10,)), dma((6, 8)), dma((3, 16)), dma((19,)),
                dma((10,)), dma((10,)), dma((num_in + 10,)), dma((num_in + 10,)),
            ],
            compiler_params=pltpu.CompilerParams(collective_id=0, has_side_effects=True, vmem_limit_bytes=67043328),
            name='denoiser_step',
        )(latents, hint_emb, in_qkv, in_proj, in_up, in_down, out_qkv, out_proj, out_up, out_down, hint_proj, zero_proj, skip_proj, final_proj)

    return jax.shard_map(device_fn, mesh=mesh, in_specs=(row_spec, row_spec) + (P(),) * 12, out_specs=row_spec, check_vma=False)
```

```python
import functools
import jax
import jax.numpy as jnp
from jax import lax
from jax.experimental import pallas as pl
from jax.experimental.pallas import tpu as pltpu
from jax.sharding import PartitionSpec as P

EPS = 1e-6
D = 2432
HALF_UP = 4864
LANES = 128
TOK = 1024
UNITS = 51
QUERIES = 256
KEYS = 512
MESH_ID = pl.DeviceIdType.MESH
BF16 = jnp.bfloat16
F32 = jnp.float32


def aligned(value, unit):
    return value if isinstance(value, int) else pl.multiple_of(value, unit)


class Chunk:
    def __init__(self, name, parts, room=0):
        self.name, self.parts, self.room = name, parts, room
        self.width = sum(width for width, _ in parts)
        self.blk = self.pos = self.sem = self.trigger = None


class WeightStream:
    def __init__(self, pre, block, post, num_blocks, buf, sem, blank):
        self.buf, self.sem, self.blank, self.num_blocks = buf, sem, blank, num_blocks
        order = []
        sems = {}

        def add(chunks, blk, kind):
            for chunk in chunks:
                item = Chunk(chunk.name, chunk.parts, chunk.room)
                item.blk, item.kind = blk, kind
                item.sem = sems.setdefault(item.name, len(sems))
                order.append(item)

        add(pre, None, 'pre')
        for blk in range(num_blocks):
            add(block, blk, 'block')
        add(post, None, 'post')
        pos = UNITS - sum(chunk.width for chunk in pre)
        holder = [None] * UNITS
        self.first = []
        self.after = {}
        self.places = {}
        for rank, item in enumerate(order):
            if pos + max(item.width, item.room) > UNITS:
                pos = 0
            item.pos, item.rank = pos, rank
            held = [holder[i] for i in range(pos, pos + item.width) if holder[i] is not None]
            holder[pos:pos + item.width] = [item] * item.width
            pos += item.width
            assert self.places.setdefault(item.name, (item.pos, item.width, item.sem)) == (item.pos, item.width, item.sem)
            if not held:
                self.first.append(item)
                continue
            last = max(held, key=lambda other: other.rank)
            self.after.setdefault(last.name, []).append((last.blk, item))
        self.num_sems = len(sems)

    def issue(self, item, blk):
        off = item.pos
        for width, source in item.parts:
            dst = self.buf.at[:, off * LANES:(off + width) * LANES]
            pltpu.make_async_copy(source(blk), dst, self.sem.at[item.sem]).start()
            off += width

    def fill(self, kind):
        for item in self.first:
            if item.kind == kind:
                self.issue(item, item.blk)

    def wait(self, name, trip, width):
        first, _, sem = self.places[(name, 0 if not isinstance(trip, int) else trip)]
        pos = first if isinstance(trip, int) else first + trip * width
        sem = sem if isinstance(trip, int) else sem + trip
        dst = self.buf.at[:, pl.ds(aligned(pos * LANES, LANES), width * LANES)]
        pltpu.make_async_copy(self.blank(width), dst, self.sem.at[sem]).wait()
        return pos

    def row(self, name, trips):
        places = [self.places[(name, trip)] for trip in range(trips)]
        first, width, sem = places[0]
        assert places == [(first + trip * width, width, sem + trip) for trip in range(trips)]

    def used_trip(self, name, trip, trips, blk):
        if isinstance(trip, int):
            self.used((name, trip), blk)
            return
        for k in range(trips):
            if self.after.get((name, k)):
                pl.when(trip == k)(functools.partial(self.used, (name, k), blk))

    def used(self, name, blk):
        todo = self.after.get(name, [])
        if blk is None or isinstance(blk, int):
            for last_blk, item in todo:
                if last_blk == blk:
                    self.issue(item, item.blk)
            return
        seen = set()
        for last_blk, item in todo:
            if item.kind == 'post':
                assert last_blk == self.num_blocks - 1
                pl.when(blk == last_blk)(lambda item=item: self.issue(item, None))
                continue
            step = item.blk - last_blk
            if (item.name, step) in seen:
                continue
            seen.add((item.name, step))
            if step == 0:
                self.issue(item, blk)
            else:
                pl.when(blk < self.num_blocks - 1)(lambda item=item: self.issue(item, blk + 1))


def matmul(lhs, rhs):
    return jnp.dot(lhs, rhs, preferred_element_type=F32)


def add_f32(left, right):
    return left.astype(F32) + right.astype(F32)


def ln_rows(src, dst, first, rows):
    for r0 in range(0, rows, 32):
        at = pl.ds(aligned(first + r0, 32), 32)
        val = src[at, :].astype(F32)
        cen = val - jnp.mean(val, axis=-1, keepdims=True)
        var = jnp.mean(cen * cen, axis=-1, keepdims=True)
        dst[at, :] = (cen * lax.rsqrt(var + EPS)).astype(BF16)


def step_kernel(num_in, lat, hint, in_qkv, in_proj, in_up, in_down, out_qkv, out_proj, out_up, out_down, hint_w, zero_w, skip_w, final_w, y_ref,
                wbuf, xl, hi, msg, u, x, act, po, ps, pin, qin, stg, o_st, a_in, vt, sb, part, rx, skp,
                wsem, init_sem, xs_sem, xr_sem, us_sem, ur_sem, qs_sem, qr_sem, as_sem, ar_sem, ps_sem, pr_sem, es_sem, er_sem):
    data_id = lax.axis_index('data')
    seq_id = lax.axis_index('seq')
    branch_id = lax.axis_index('branch')
    core = branch_id % 2
    row_y = branch_id // 2
    side = seq_id // 2
    quad = 2 * row_y + seq_id % 2
    chip = 4 * side + quad

    def device(side_id, quad_id, core_id):
        return (data_id, 2 * side_id + quad_id % 2, 2 * (quad_id // 2) + core_id)

    peer = device(side, quad, 1 - core)
    partner = device(1 - side, quad, core)

    def remote(src, dst, send, recv, dev):
        return pltpu.make_async_remote_copy(src_ref=src, dst_ref=dst, send_sem=send, recv_sem=recv, device_id=dev, device_id_type=MESH_ID)

    def layout(is_in):
        n_chips = 4 if is_in else 8
        me = quad if is_in else chip
        bits = 2 if is_in else 3

        def extra_dest(idx):
            return 2 * idx + core if is_in else 1 + 5 * idx + 3 * core

        def combo(j):
            trip, odd = j // 2, j % 2
            extra = trip // 4
            half = n_chips // 2
            rel = (half - 1) - trip % half
            top = me // 2
            prim = (top + rel) % 2 if is_in else 2 * ((top // 2 + rel // 2) % 2) + (top + rel) % 2
            prim = 2 * prim + odd
            slot_p = trip // half
            idx = odd - core
            dest = (1 - extra) * prim + extra * extra_dest(idx)
            slot = (1 - extra) * slot_p + extra * (8 // n_chips)
            num = (1 - extra) * (10 * core + slot_p * n_chips + prim) + extra * (10 * core + 8 + idx)
            return dest, slot, num, extra * core * (1 - odd) == 0

        def owner(num):
            plane, j = num // 10, num % 10
            extra = j // 8
            left = 2 * (j - 8) + plane if is_in else 1 + 5 * (j - 8) + 3 * plane
            return plane, (1 - extra) * (j % n_chips) + extra * left

        return n_chips, me, combo, owner, extra_dest

    def chip_device(is_in, idx, core_id):
        return device(side, idx, core_id) if is_in else device(idx // 4, idx % 4, core_id)

    num_blocks = num_in + 1
    num_out = num_in

    def cols(start):
        return pl.ds(aligned(start, LANES), LANES)

    def wide(start, width):
        return pl.ds(aligned(start, LANES), width * LANES)

    WIDE = (8, 8, 3)
    NARROW = (4, 4, 4, 4, 3)

    def square(name, source, widths=WIDE):
        out, first = [], 0
        for trip, width in enumerate(widths):
            out.append(Chunk((name, trip), [(width, lambda blk, first=first, width=width: source(blk, wide(first * LANES, width)))], 16 if trip == 0 else 0))
            first += width
        return out

    def qkv_chunks(name, combo, source):
        out = []
        for trip in range(5):
            num = combo(2 * trip)[2]
            out.append(Chunk((name, trip), [(2, lambda blk, num=num, part=part: source(blk, wide(part * D + num * LANES, 2))) for part in range(3)], 30 if trip == 0 else 0))
        return out

    UP_TRIPS = (8, 8, 8, 8, 6)
    DOWN_TRIPS = (4, 4, 4, 4, 3)

    def up_chunks(name, source):
        out, first = [], 0
        for trip, width in enumerate(UP_TRIPS):
            out.append(Chunk((name, trip), [(width, lambda blk, first=first, width=width: source(blk, wide(core * HALF_UP + first * LANES, width)))], 32 if trip == 0 else 0))
            first += width
        return out

    def down_chunks(name, source):
        out, first = [], 0
        for trip, width in enumerate(DOWN_TRIPS):
            out.append(Chunk((name, trip), [
                (width, lambda blk, first=first, width=width, k=k: source(blk, pl.ds(aligned(core * HALF_UP + k * D, LANES), D), wide(first * LANES, width)))
                for k in range(2)], 32 if trip == 0 else 0))
            first += width
        return out

    in_combo, out_combo = layout(True)[2], layout(False)[2]
    pre = square('hint', lambda blk, c: hint_w.at[:, c])
    block = (qkv_chunks('in_qkv', in_combo, lambda blk, c: in_qkv.at[side, blk, :, c])
             + square('in_zero', lambda blk, c: zero_w.at[(blk + num_in) % num_blocks, :, c], NARROW)
             + square('in_proj', lambda blk, c: in_proj.at[side, blk, :, c])
             + up_chunks('in_up', lambda blk, c: in_up.at[side, blk, :, c])
             + down_chunks('in_down', lambda blk, r, c: in_down.at[side, blk, r, c]))

    def skip_square(idx, half):
        return square(('skip', idx, half), lambda blk, c: skip_w.at[idx, pl.ds(half * D, D), c], NARROW if half else WIDE)

    post = square('zero', lambda blk, c: zero_w.at[num_in, :, c]) + skip_square(0, 1) + skip_square(0, 0)
    for idx in range(num_out):
        post += qkv_chunks(('qkv', idx), out_combo, lambda blk, c, idx=idx: out_qkv.at[idx, :, c])
        if idx + 1 < num_out:
            post += skip_square(idx + 1, 1)
        post += square(('proj', idx), lambda blk, c, idx=idx: out_proj.at[idx, :, c])
        post += up_chunks(('up', idx), lambda blk, c, idx=idx: out_up.at[idx, :, c])
        post += down_chunks(('down', idx), lambda blk, r, c, idx=idx: out_down.at[idx, r, c])
        if idx + 1 < num_out:
            post += skip_square(idx + 1, 0)
    post += square('final', lambda blk, c: final_w.at[:, c])
    stream = WeightStream(pre, block, post, num_blocks, wbuf, wsem, lambda width: in_up.at[0, 0, :, 0:width * LANES])

    def columns(pos, width):
        return wbuf[:, pl.ds(aligned(pos * LANES, LANES), width * LANES)]

    def mm(blk, name, looped, widths, lhs, emit, done=None, k_subs=1):
        stream.row(name, looped)

        def trip(t, col, width):
            pos = stream.wait(name, t, width * k_subs)
            for first in range(0, width, 2):
                size = min(2, width - first)
                subs = [columns(pos + k * width + first, size) for k in range(k_subs)]
                rhs = subs[0] if k_subs == 1 else jnp.concatenate(subs, axis=0)
                emit(aligned(col + first * LANES, LANES), size * LANES, matmul(lhs(), rhs))
            if done is not None:
                done(aligned(col, LANES), width * LANES)
            stream.used_trip(name, t, looped, blk)

        pl.loop(0, looped)(lambda t: trip(t, t * (widths[0] * LANES), widths[0]))
        col = looped * widths[0] * LANES
        for t in range(looped, len(widths)):
            trip(t, col, widths[t])
            col += widths[t] * LANES

    def mm_square(blk, name, lhs, emit, done=None, widths=WIDE):
        mm(blk, name, len(widths) - 1, widths, lhs, emit, done)

    def mm_up(blk, name, lhs, emit):
        mm(blk, name, 4, UP_TRIPS, lhs, emit)

    def mm_down(blk, name, lhs, emit, done):
        mm(blk, name, 4, DOWN_TRIPS, lhs, emit, done, 2)

    def each(widths, fn):
        col = 0
        for width in widths:
            fn(col, width * LANES)
            col += width * LANES

    scope = jax.named_scope
    get_lat = pltpu.make_async_copy(lat.at[0], xl, init_sem.at[0])
    get_hint = pltpu.make_async_copy(hint.at[0], hi, init_sem.at[1])
    with scope('barrier'):
        get_hint.start()
        get_lat.start()
        stream.fill('pre')
        barrier = pltpu.get_barrier_semaphore()
        my_index = seq_id * 4 + branch_id
        for k in range(1, 16):
            other = (my_index + k) % 16
            pl.semaphore_signal(barrier, inc=1, device_id=(data_id, other // 4, other % 4), device_id_type=MESH_ID)
        pl.semaphore_wait(barrier, 15)
        get_lat.wait()
        get_hint.wait()

    mine = pl.ds(pl.multiple_of(side * 64, 64), 64)
    theirs = pl.ds(pl.multiple_of((1 - side) * 64, 64), 64)

    def swap_copy(col, width):
        return remote(msg.at[:, pl.ds(col, width)], u.at[mine, pl.ds(col, width)], us_sem.at[col // 1024], ur_sem.at[col // 1024], partner)

    def emit_hint(col, width, acc):
        base_in = xl[:, pl.ds(col, width)]
        control_in = add_f32(base_in, acc.astype(BF16)).astype(BF16)
        is_base = side == 0
        u[mine, pl.ds(col, width)] = jnp.where(is_base, base_in, control_in)
        msg[:, pl.ds(col, width)] = jnp.where(is_base, control_in, base_in)

    with scope('hint'):
        mm_square(None, 'hint', lambda: hi[...], emit_hint, lambda col, width: swap_copy(col, width).start())
        stream.fill('block')
    def exchange_half(half, first, size, rows):
        ln_rows(u, x, first, size)
        send = remote(x.at[pl.ds(first, size)], x.at[pl.ds(aligned(first + rows, 32), size)], xs_sem.at[half], xr_sem.at[half], peer)
        send.start()
        return send

    def exchange_rows(rows):
        sends = [exchange_half(half, half * (rows // 2), rows // 2, rows) for half in range(2)]
        for send in sends:
            send.wait_recv()
        return sends

    def run_block(is_in, blk, names, bank, fill_in, before_proj):
        rows = 128 if is_in else 64
        chip_rows = 2 * rows
        n_chips, me, combo, owner, extra_dest = layout(is_in)
        extra_slot = 8 // n_chips
        qkv_name, proj_name, up_name, down_name = names

        def chunk(idx, size):
            return pl.ds(aligned(idx * size, size), size)

        def piece_copy(j, dest, slot):
            at = 3 * bank + slot
            return remote(stg.at[j, pl.ds(0, chip_rows)], qin.at[at, chunk(me, chip_rows)], qs_sem.at[j], qr_sem.at[at, me], chip_device(is_in, dest, core))

        def qkv_trip(trip):
            pos = stream.wait(qkv_name, trip, 6)
            for part in range(3):
                both = matmul(x[0:chip_rows, :], columns(pos + 2 * part, 2)).astype(BF16)
                stg[2 * trip, 0:chip_rows, part * LANES:(part + 1) * LANES] = both[:, 0:LANES]
                stg[2 * trip + 1, 0:chip_rows, part * LANES:(part + 1) * LANES] = both[:, LANES:2 * LANES]
            for j in (2 * trip, 2 * trip + 1):
                dest, slot, num, valid = combo(j)

                @pl.when(jnp.logical_and(valid, dest != me))
                def _(j=j, dest=dest, slot=slot):
                    piece_copy(j, dest, slot).start()

                @pl.when(jnp.logical_and(valid, dest == me))
                def _(j=j, slot=slot):
                    qin[3 * bank + slot, chunk(me, chip_rows), :] = stg[j, 0:chip_rows, :]

            stream.used_trip(qkv_name, trip, 5, blk)

        def norm_and_qkv():
            with scope('ln1'):
                sends = exchange_rows(rows)
            with scope('qkv'):
                stream.row(qkv_name, 5)
                pl.loop(0, 5)(qkv_trip)
            for send in sends:
                send.wait_send()

        if is_in:
            pl.when(blk > 0)(norm_and_qkv)
        else:
            norm_and_qkv()
        with scope('fill'):
            fill_in()

        holds = [(extra_dest(0) == me).astype(jnp.int32), jnp.logical_and(extra_dest(1) == me, core == 0).astype(jnp.int32)]
        num_slots = extra_slot + holds[0] + holds[1]

        def slot_pair(slot):
            extra = slot // extra_slot
            return (1 - extra) * (10 * core + slot * n_chips + me) + extra * (10 * core + 8 + holds[1])

        per_chunk = QUERIES // chip_rows

        def query_chunk(i):
            return (me // per_chunk + 1 + i) % (TOK // QUERIES)

        def send_copies(slot, i):
            copies = []
            num = slot_pair(slot)
            first = query_chunk(i) * per_chunk
            chips = [(first + n, True) for n in range(per_chunk)]
            if i == TOK // QUERIES - 1:
                chips = [(me, False)] if per_chunk == 1 else [(me + 1 - 2 * (me % 2), True), (me, False)]
            for n, (idx, other) in enumerate(chips):
                for which in range(2):
                    if not other and which == 0:
                        continue
                    to_core = core if which == 0 else 1 - core
                    src = o_st.at[slot, pl.ds(pl.multiple_of(idx * chip_rows + which * rows, rows), rows)]
                    copies.append(remote(src, a_in.at[pl.ds(0, rows), cols(num * LANES)], as_sem.at[slot, 4 * i + 2 * n + which], ar_sem.at[num], chip_device(is_in, idx, to_core)))
            return copies

        def attend(slot):
            at = 3 * bank + slot
            with scope('att_wait'):
                for k in range(1, n_chips):
                    src = (me + k) % n_chips
                    remote(stg.at[0, pl.ds(0, chip_rows)], qin.at[at, chunk(src, chip_rows)], qs_sem.at[0], qr_sem.at[at, src], peer).wait_recv()
            vt[...] = qin[at, :, 2 * LANES:3 * LANES].T
            low = lax.broadcasted_iota(jnp.int32, (QUERIES, LANES), 1) < 64

            def trip(now, after, top):
                top_next = total = out_a = out_b = None
                if after is not None:
                    q_pair = (qin[at, chunk(query_chunk(after), QUERIES), 0:LANES].astype(F32) * 0.125).astype(BF16)
                    none = jnp.zeros_like(q_pair)
                    q_both = jnp.concatenate([jnp.where(low, q_pair, none), jnp.where(low, none, q_pair)], axis=0)
                for k0 in range(0, TOK, KEYS):
                    keys = slice(k0, k0 + KEYS)
                    if after is not None:
                        score = lax.dot_general(qin[at, keys, LANES:2 * LANES], q_both, (((1,), (1,)), ((), ())), preferred_element_type=F32)
                        sb[after % 2, keys, :] = score
                        part_top = jnp.max(score.reshape(KEYS // 8, 8, 2 * QUERIES), axis=0)
                        top_next = part_top if top_next is None else jnp.maximum(top_next, part_top)
                    if now is not None:
                        weight = jnp.exp(sb[now % 2, keys, :] - top)
                        part_sum = jnp.sum(weight.reshape(KEYS // 8, 8, 2 * QUERIES), axis=0)
                        total = part_sum if total is None else total + part_sum
                        prob = weight.astype(BF16)
                        term_a = matmul(vt[0:64, keys], prob[:, 0:QUERIES])
                        term_b = matmul(vt[64:128, keys], prob[:, QUERIES:2 * QUERIES])
                        out_a = term_a if out_a is None else out_a + term_a
                        out_b = term_b if out_b is None else out_b + term_b
                if now is not None:
                    inv = 1.0 / jnp.sum(total, axis=0, keepdims=True)
                    mixed = jnp.concatenate([out_a * inv[:, 0:QUERIES], out_b * inv[:, QUERIES:2 * QUERIES]], axis=0)
                    o_st[slot, chunk(query_chunk(now), QUERIES), :] = mixed.T.astype(BF16)
                    for copy in send_copies(slot, now):
                        copy.start()
                return None if after is None else jnp.max(top_next, axis=0, keepdims=True)

            last = TOK // QUERIES - 1
            top = trip(None, 0, None)
            for i in range(last):
                top = trip(i, i + 1, top)
            trip(last, None, top)
            a_in[0:rows, cols(slot_pair(slot) * LANES)] = o_st[slot, pl.ds(pl.multiple_of(me * chip_rows, chip_rows), rows), :]

        with scope('att'):
            pl.loop(0, num_slots)(attend)

        with scope('await'):
            @pl.loop(0, 10)
            def _(j):
                dest, slot, num, valid = combo(j)

                @pl.when(jnp.logical_and(valid, dest != me))
                def _():
                    piece_copy(j, dest, slot).wait_send()

            @pl.loop(0, 19)
            def _(num):
                plane, dest = owner(num)

                @pl.when(jnp.logical_not(jnp.logical_and(core == plane, me == dest)))
                def _():
                    remote(o_st.at[0, pl.ds(0, rows)], a_in.at[pl.ds(0, rows), cols(num * LANES)], as_sem.at[0, 0], ar_sem.at[num], peer).wait_recv()

            before_proj()

        def emit_proj(col, width, acc):
            u[0:rows, pl.ds(col, width)] = add_f32(u[0:rows, pl.ds(col, width)], acc.astype(BF16)).astype(BF16)

        with scope('proj'):
            mm_square(blk, proj_name, lambda: a_in[0:rows, :], emit_proj)

            @pl.loop(0, num_slots)
            def _(slot):
                for i in range(TOK // QUERIES):
                    for copy in send_copies(slot, i):
                        copy.wait_send()

        with scope('ln2'):
            sends = exchange_rows(rows)

        def emit_up(col, width, acc):
            hidden = acc.astype(BF16).astype(F32)
            act[0:chip_rows, pl.ds(col, width)] = jax.nn.gelu(hidden).astype(BF16)

        with scope('up'):
            mm_up(blk, up_name, lambda: x[0:chip_rows, :], emit_up)
            for send in sends:
                send.wait_send()

        def partial_copy(col, width):
            tile = col // 512
            return remote(ps.at[pl.ds(0, rows), pl.ds(col, width)], pin.at[pl.ds(0, rows), pl.ds(col, width)], ps_sem.at[tile], pr_sem.at[tile], peer)

        def emit_down(col, width, acc):
            po[0:rows, pl.ds(col, width)] = acc[0:rows]
            ps[0:rows, pl.ds(col, width)] = acc[rows:chip_rows]

        with scope('down'):
            mm_down(blk, down_name, lambda: act[0:chip_rows, :], emit_down, lambda col, width: partial_copy(col, width).start())

        def finish(col, width):
            partial_copy(col, width).wait()
            total = (po[0:rows, pl.ds(col, width)] + pin[0:rows, pl.ds(col, width)]).astype(BF16)
            u[0:rows, pl.ds(col, width)] = add_f32(u[0:rows, pl.ds(col, width)], total).astype(BF16)

        with scope('fin'):
            pl.loop(0, 4)(lambda t: finish(aligned(t * 512, 512), 512))
            finish(4 * 512, 384)

    def make_part(blk, name, idx, after=None, widths=WIDE):
        def emit(col, width, acc):
            part[idx, :, pl.ds(col, width)] = jnp.where(side == 0, u[:, pl.ds(col, width)], acc.astype(BF16))
        mm_square(blk, name, lambda: u[...], emit, after, widths)

    def part_copy(idx):
        return remote(part.at[idx, theirs], rx.at[idx], es_sem.at[idx], er_sem.at[idx], partner)

    def mid_copy(col, width):
        tile = num_in + col // 1024
        return remote(part.at[num_in, theirs, pl.ds(col, width)], rx.at[num_in, :, pl.ds(col, width)], es_sem.at[tile], er_sem.at[tile], partner)

    nothing = lambda: None

    def first_qkv():
        n_chips, me, combo, _, _ = layout(True)

        def piece_copies(j, dest, slot, off):
            return [remote(stg.at[j, pl.ds(pl.multiple_of(off + at, 64), 64)], qin.at[slot, pl.ds(pl.multiple_of(me * 256 + off + at, 64), 64)],
                           qs_sem.at[j], qr_sem.at[slot, me], device(side, dest, core)) for at in (0, 128)]

        stream.row('in_qkv', 5)
        base = stream.places[('in_qkv', 0)][0]

        @pl.loop(0, 2)
        def _(half):
            off = (side + half) % 2 * 64

            @pl.when(half == 1)
            def _():
                each(WIDE, lambda col, width: swap_copy(col, width).wait())

            send = exchange_half(half, pl.multiple_of(off, 64), 64, 128)
            send.wait_recv()
            own, other = pl.ds(pl.multiple_of(off, 64), 64), pl.ds(pl.multiple_of(128 + off, 64), 64)

            @pl.loop(0, 5)
            def _(t):
                pl.when(half == 0)(lambda: (stream.wait('in_qkv', t, 6), None)[1])
                for part in range(3):
                    lhs = jnp.concatenate([x[own, :], x[other, :]], axis=0)
                    both = matmul(lhs, columns(base + 6 * t + 2 * part, 2)).astype(BF16)
                    for odd in range(2):
                        stg[2 * t + odd, own, part * LANES:(part + 1) * LANES] = both[0:64, odd * LANES:(odd + 1) * LANES]
                        stg[2 * t + odd, other, part * LANES:(part + 1) * LANES] = both[64:128, odd * LANES:(odd + 1) * LANES]
                for j in (2 * t, 2 * t + 1):
                    dest, slot, num, valid = combo(j)

                    @pl.when(jnp.logical_and(valid, dest != me))
                    def _(j=j, dest=dest, slot=slot):
                        for copy in piece_copies(j, dest, slot, off):
                            copy.start()

                    @pl.when(jnp.logical_and(valid, dest == me))
                    def _(j=j, slot=slot):
                        for at in (0, 128):
                            qin[slot, pl.ds(pl.multiple_of(me * 256 + off + at, 64), 64), :] = stg[j, pl.ds(pl.multiple_of(off + at, 64), 64), :]
                pl.when(half == 1)(lambda: stream.used_trip('in_qkv', t, 5, 0))

            send.wait_send()

    first_qkv()

    @pl.loop(0, num_blocks)
    def _(blk):
        def send_part():
            pl.when(blk > 0)(lambda: part_copy(blk - 1).start())

        run_block(True, blk, ('in_qkv', 'in_proj', 'in_up', 'in_down'), blk % 2, lambda: make_part(blk, 'in_zero', (blk + num_in) % num_blocks, widths=NARROW), send_part)

    with scope('midpart'):
        make_part(None, 'zero', num_in, lambda col, width: mid_copy(col, width).start())
        for idx in range(num_in):
            part_copy(idx).wait()
            rx[idx] = add_f32(part[idx, mine, :], rx[idx]).astype(BF16)

    def skip_part(blk):
        def emit(col, width, acc):
            skp[:, pl.ds(col, width)] = acc
        mm_square(None, ('skip', blk, 1), lambda: rx[num_in - 1 - blk], emit, widths=NARROW)

    def merge(blk):
        def emit(col, width, acc):
            msg[:, pl.ds(col, width)] = (skp[:, pl.ds(col, width)] + acc).astype(BF16)
        mm_square(None, ('skip', blk, 0), lambda: u[0:64, :], emit)
        u[0:64, :] = msg[...]

    with scope('skip0'):
        skip_part(0)

    def mid_sum(col, width):
        mid_copy(col, width).wait()
        u[0:64, pl.ds(col, width)] = add_f32(part[num_in, mine, pl.ds(col, width)], rx[num_in, :, pl.ds(col, width)]).astype(BF16)

    with scope('midwait'):
        each(WIDE, mid_sum)
    for blk in range(num_out):
        with scope('merge'):
            merge(blk)
        run_block(False, None, (('qkv', blk), ('proj', blk), ('up', blk), ('down', blk)), (num_blocks + blk) % 2, functools.partial(skip_part, blk + 1) if blk + 1 < num_out else nothing, nothing)

    def emit_final(col, width, acc):
        y_ref[0, :, pl.ds(col, width)] = acc.astype(BF16)

    with scope('final'):
        ln_rows(u, x, 0, 64)
        mm_square(None, 'final', lambda: x[0:64, :], emit_final)


def solution(mesh):
    row_spec = P('data', ('seq', 'branch'), None)

    def device_fn(latents, hint_emb, in_qkv, in_proj, in_up, in_down, out_qkv, out_proj, out_up, out_down, hint_proj, zero_proj, skip_proj, final_proj):
        num_in = out_qkv.shape[0]
        in_proj = in_proj.reshape(2, num_in + 1, D, D)
        out_proj = out_proj.reshape(num_in, D, D)
        anywhere = pl.BlockSpec(memory_space=pl.ANY)
        dma = pltpu.SemaphoreType.DMA
        return pl.pallas_call(
            functools.partial(step_kernel, num_in),
            out_shape=jax.ShapeDtypeStruct((1, 64, D), BF16),
            in_specs=[anywhere] * 14,
            out_specs=pl.BlockSpec(memory_space=pltpu.VMEM),
            scratch_shapes=[
                pltpu.VMEM((D, UNITS * LANES), BF16),
                pltpu.VMEM((64, D), BF16),
                pltpu.VMEM((64, D), BF16),
                pltpu.VMEM((64, D), BF16),
                pltpu.VMEM((128, D), BF16),
                pltpu.VMEM((256, D), BF16),
                pltpu.VMEM((256, HALF_UP), BF16),
                pltpu.VMEM((128, D), F32),
                pltpu.VMEM((128, D), F32),
                pltpu.VMEM((128, D), F32),
                pltpu.VMEM((6, TOK, 3 * LANES), BF16),
                pltpu.VMEM((10, 256, 3 * LANES), BF16),
                pltpu.VMEM((3, TOK, LANES), BF16),
                pltpu.VMEM((128, D), BF16),
                pltpu.VMEM((LANES, TOK), BF16),
                pltpu.VMEM((2, TOK, 2 * QUERIES), F32),
                pltpu.VMEM((num_in + 1, 128, D), BF16),
                pltpu.VMEM((num_in + 1, 64, D), BF16),
                pltpu.VMEM((64, D), F32),
                dma((100,)), dma((2,)), dma((2,)), dma((2,)), dma((10,)), dma((10,)),
                dma((10,)), dma((6, 8)), dma((3, 16)), dma((19,)),
                dma((10,)), dma((10,)), dma((num_in + 10,)), dma((num_in + 10,)),
            ],
            compiler_params=pltpu.CompilerParams(collective_id=0, has_side_effects=True, vmem_limit_bytes=67043328),
            name='denoiser_step',
        )(latents, hint_emb, in_qkv, in_proj, in_up, in_down, out_qkv, out_proj, out_up, out_down, hint_proj, zero_proj, skip_proj, final_proj)

    return jax.shard_map(device_fn, mesh=mesh, in_specs=(row_spec, row_spec) + (P(),) * 12, out_specs=row_spec, check_vma=False)
```

```python
import functools
import jax
import jax.numpy as jnp
from jax import lax
from jax.experimental import pallas as pl
from jax.experimental.pallas import tpu as pltpu
from jax.sharding import PartitionSpec as P

EPS = 1e-6
D = 2432
HALF_UP = 4864
LANES = 128
TOK = 1024
UNITS = 51
QUERIES = 256
KEYS = 512
MESH_ID = pl.DeviceIdType.MESH
BF16 = jnp.bfloat16
F32 = jnp.float32


def aligned(value, unit):
    return value if isinstance(value, int) else pl.multiple_of(value, unit)


class Chunk:
    def __init__(self, name, parts, room=0):
        self.name, self.parts, self.room = name, parts, room
        self.width = sum(width for width, _ in parts)
        self.blk = self.pos = self.sem = self.trigger = None


class WeightStream:
    def __init__(self, pre, block, post, num_blocks, buf, sem, blank):
        self.buf, self.sem, self.blank, self.num_blocks = buf, sem, blank, num_blocks
        order = []
        sems = {}

        def add(chunks, blk, kind):
            for chunk in chunks:
                item = Chunk(chunk.name, chunk.parts, chunk.room)
                item.blk, item.kind = blk, kind
                item.sem = sems.setdefault(item.name, len(sems))
                order.append(item)

        add(pre, None, 'pre')
        for blk in range(num_blocks):
            add(block, blk, 'block')
        add(post, None, 'post')
        pos = UNITS - sum(chunk.width for chunk in pre)
        holder = [None] * UNITS
        self.first = []
        self.after = {}
        self.places = {}
        for rank, item in enumerate(order):
            if pos + max(item.width, item.room) > UNITS:
                pos = 0
            item.pos, item.rank = pos, rank
            held = [holder[i] for i in range(pos, pos + item.width) if holder[i] is not None]
            holder[pos:pos + item.width] = [item] * item.width
            pos += item.width
            assert self.places.setdefault(item.name, (item.pos, item.width, item.sem)) == (item.pos, item.width, item.sem)
            if not held:
                self.first.append(item)
                continue
            last = max(held, key=lambda other: other.rank)
            self.after.setdefault(last.name, []).append((last.blk, item))
        self.num_sems = len(sems)

    def issue(self, item, blk):
        off = item.pos
        for width, source in item.parts:
            dst = self.buf.at[:, off * LANES:(off + width) * LANES]
            pltpu.make_async_copy(source(blk), dst, self.sem.at[item.sem]).start()
            off += width

    def fill(self, kind):
        for item in self.first:
            if item.kind == kind:
                self.issue(item, item.blk)

    def wait(self, name, trip, width):
        first, _, sem = self.places[(name, 0 if not isinstance(trip, int) else trip)]
        pos = first if isinstance(trip, int) else first + trip * width
        sem = sem if isinstance(trip, int) else sem + trip
        dst = self.buf.at[:, pl.ds(aligned(pos * LANES, LANES), width * LANES)]
        pltpu.make_async_copy(self.blank(width), dst, self.sem.at[sem]).wait()
        return pos

    def row(self, name, trips):
        places = [self.places[(name, trip)] for trip in range(trips)]
        first, width, sem = places[0]
        assert places == [(first + trip * width, width, sem + trip) for trip in range(trips)]

    def used_trip(self, name, trip, trips, blk):
        if isinstance(trip, int):
            self.used((name, trip), blk)
            return
        for k in range(trips):
            if self.after.get((name, k)):
                pl.when(trip == k)(functools.partial(self.used, (name, k), blk))

    def used(self, name, blk):
        todo = self.after.get(name, [])
        if blk is None or isinstance(blk, int):
            for last_blk, item in todo:
                if last_blk == blk:
                    self.issue(item, item.blk)
            return
        seen = set()
        for last_blk, item in todo:
            if item.kind == 'post':
                assert last_blk == self.num_blocks - 1
                pl.when(blk == last_blk)(lambda item=item: self.issue(item, None))
                continue
            step = item.blk - last_blk
            if (item.name, step) in seen:
                continue
            seen.add((item.name, step))
            if step == 0:
                self.issue(item, blk)
            else:
                pl.when(blk < self.num_blocks - 1)(lambda item=item: self.issue(item, blk + 1))


def matmul(lhs, rhs):
    return jnp.dot(lhs, rhs, preferred_element_type=F32)


def add_f32(left, right):
    return left.astype(F32) + right.astype(F32)


def ln_rows(src, dst, first, rows):
    for r0 in range(0, rows, 32):
        at = pl.ds(aligned(first + r0, 32), 32)
        val = src[at, :].astype(F32)
        cen = val - jnp.mean(val, axis=-1, keepdims=True)
        var = jnp.mean(cen * cen, axis=-1, keepdims=True)
        dst[at, :] = (cen * lax.rsqrt(var + EPS)).astype(BF16)


def step_kernel(num_in, lat, hint, in_qkv, in_proj, in_up, in_down, out_qkv, out_proj, out_up, out_down, hint_w, zero_w, skip_w, final_w, y_ref,
                wbuf, xl, hi, msg, u, x, act, po, ps, pin, qin, stg, o_st, a_in, vt, sb, part, rx, skp,
                wsem, init_sem, xs_sem, xr_sem, us_sem, ur_sem, qs_sem, qr_sem, as_sem, ar_sem, ps_sem, pr_sem, es_sem, er_sem):
    data_id = lax.axis_index('data')
    seq_id = lax.axis_index('seq')
    branch_id = lax.axis_index('branch')
    core = branch_id % 2
    row_y = branch_id // 2
    side = seq_id // 2
    quad = 2 * row_y + seq_id % 2
    chip = 4 * side + quad

    def device(side_id, quad_id, core_id):
        return (data_id, 2 * side_id + quad_id % 2, 2 * (quad_id // 2) + core_id)

    peer = device(side, quad, 1 - core)
    partner = device(1 - side, quad, core)

    def remote(src, dst, send, recv, dev):
        return pltpu.make_async_remote_copy(src_ref=src, dst_ref=dst, send_sem=send, recv_sem=recv, device_id=dev, device_id_type=MESH_ID)

    def layout(is_in):
        n_chips = 4 if is_in else 8
        me = quad if is_in else chip
        bits = 2 if is_in else 3

        def extra_dest(idx):
            return 2 * idx + core if is_in else 1 + 5 * idx + 3 * core

        def combo(j):
            trip, odd = j // 2, j % 2
            extra = trip // 4
            half = n_chips // 2
            rel = (half - 1) - trip % half
            top = me // 2
            prim = (top + rel) % 2 if is_in else 2 * ((top // 2 + rel // 2) % 2) + (top + rel) % 2
            prim = 2 * prim + odd
            slot_p = trip // half
            idx = odd - core
            dest = (1 - extra) * prim + extra * extra_dest(idx)
            slot = (1 - extra) * slot_p + extra * (8 // n_chips)
            num = (1 - extra) * (10 * core + slot_p * n_chips + prim) + extra * (10 * core + 8 + idx)
            return dest, slot, num, extra * core * (1 - odd) == 0

        def owner(num):
            plane, j = num // 10, num % 10
            extra = j // 8
            left = 2 * (j - 8) + plane if is_in else 1 + 5 * (j - 8) + 3 * plane
            return plane, (1 - extra) * (j % n_chips) + extra * left

        return n_chips, me, combo, owner, extra_dest

    def chip_device(is_in, idx, core_id):
        return device(side, idx, core_id) if is_in else device(idx // 4, idx % 4, core_id)

    num_blocks = num_in + 1
    num_out = num_in

    def cols(start):
        return pl.ds(aligned(start, LANES), LANES)

    def wide(start, width):
        return pl.ds(aligned(start, LANES), width * LANES)

    WIDE = (8, 8, 3)
    NARROW = (4, 4, 4, 4, 3)

    def square(name, source, widths=WIDE):
        out, first = [], 0
        for trip, width in enumerate(widths):
            out.append(Chunk((name, trip), [(width, lambda blk, first=first, width=width: source(blk, wide(first * LANES, width)))], 19 if trip == 0 else 0))
            first += width
        return out

    def qkv_chunks(name, combo, source):
        out = []
        for trip in range(5):
            num = combo(2 * trip)[2]
            out.append(Chunk((name, trip), [(2, lambda blk, num=num, part=part: source(blk, wide(part * D + num * LANES, 2))) for part in range(3)], 30 if trip == 0 else 0))
        return out

    UP_TRIPS = (8, 8, 8, 8, 6)
    DOWN_TRIPS = (4, 4, 4, 4, 3)

    def up_chunks(name, source):
        out, first = [], 0
        for trip, width in enumerate(UP_TRIPS):
            out.append(Chunk((name, trip), [(width, lambda blk, first=first, width=width: source(blk, wide(core * HALF_UP + first * LANES, width)))], 32 if trip == 0 else 0))
            first += width
        return out

    def down_chunks(name, source):
        out, first = [], 0
        for trip, width in enumerate(DOWN_TRIPS):
            out.append(Chunk((name, trip), [
                (width, lambda blk, first=first, width=width, k=k: source(blk, pl.ds(aligned(core * HALF_UP + k * D, LANES), D), wide(first * LANES, width)))
                for k in range(2)], 32 if trip == 0 else 0))
            first += width
        return out

    in_combo, out_combo = layout(True)[2], layout(False)[2]
    pre = square('hint', lambda blk, c: hint_w.at[:, c])
    block = (qkv_chunks('in_qkv', in_combo, lambda blk, c: in_qkv.at[side, blk, :, c])
             + square('in_zero', lambda blk, c: zero_w.at[(blk + num_in) % num_blocks, :, c], NARROW)
             + square('in_proj', lambda blk, c: in_proj.at[side, blk, :, c], NARROW)
             + up_chunks('in_up', lambda blk, c: in_up.at[side, blk, :, c])
             + down_chunks('in_down', lambda blk, r, c: in_down.at[side, blk, r, c]))

    def skip_square(idx, half):
        return square(('skip', idx, half), lambda blk, c: skip_w.at[idx, pl.ds(half * D, D), c], NARROW if half else WIDE)

    post = square('zero', lambda blk, c: zero_w.at[num_in, :, c]) + skip_square(0, 1) + skip_square(0, 0)
    for idx in range(num_out):
        post += qkv_chunks(('qkv', idx), out_combo, lambda blk, c, idx=idx: out_qkv.at[idx, :, c])
        if idx + 1 < num_out:
            post += skip_square(idx + 1, 1)
        post += square(('proj', idx), lambda blk, c, idx=idx: out_proj.at[idx, :, c], NARROW)
        post += up_chunks(('up', idx), lambda blk, c, idx=idx: out_up.at[idx, :, c])
        post += down_chunks(('down', idx), lambda blk, r, c, idx=idx: out_down.at[idx, r, c])
        if idx + 1 < num_out:
            post += skip_square(idx + 1, 0)
    post += square('final', lambda blk, c: final_w.at[:, c])
    stream = WeightStream(pre, block, post, num_blocks, wbuf, wsem, lambda width: in_up.at[0, 0, :, 0:width * LANES])

    def columns(pos, width, pick=None):
        cut = pl.ds(aligned(pos * LANES, LANES), width * LANES)
        if pick is None:
            return wbuf[:, cut]
        return jnp.concatenate([wbuf[first:last, cut] for first, last in pick], axis=0)

    def mm(blk, name, looped, widths, lhs, emit, done=None, k_subs=1, pick=None):
        stream.row(name, looped)

        def trip(t, col, width):
            pos = stream.wait(name, t, width * k_subs)
            for first in range(0, width, 2):
                size = min(2, width - first)
                subs = [columns(pos + k * width + first, size, pick) for k in range(k_subs)]
                rhs = subs[0] if k_subs == 1 else jnp.concatenate(subs, axis=0)
                emit(aligned(col + first * LANES, LANES), size * LANES, matmul(lhs(), rhs))
            if done is not None:
                done(aligned(col, LANES), width * LANES)
            if pick is None:
                stream.used_trip(name, t, looped, blk)

        pl.loop(0, looped)(lambda t: trip(t, t * (widths[0] * LANES), widths[0]))
        col = looped * widths[0] * LANES
        for t in range(looped, len(widths)):
            trip(t, col, widths[t])
            col += widths[t] * LANES

    def mm_square(blk, name, lhs, emit, done=None, widths=WIDE):
        mm(blk, name, len(widths) - 1, widths, lhs, emit, done)

    def mm_up(blk, name, lhs, emit):
        mm(blk, name, 4, UP_TRIPS, lhs, emit)

    def mm_down(blk, name, lhs, emit, done):
        mm(blk, name, 4, DOWN_TRIPS, lhs, emit, done, 2)

    def each(widths, fn):
        col = 0
        for width in widths:
            fn(col, width * LANES)
            col += width * LANES

    scope = jax.named_scope
    get_lat = pltpu.make_async_copy(lat.at[0], xl, init_sem.at[0])
    get_hint = pltpu.make_async_copy(hint.at[0], hi, init_sem.at[1])
    with scope('barrier'):
        get_hint.start()
        get_lat.start()
        stream.fill('pre')
        barrier = pltpu.get_barrier_semaphore()
        my_index = seq_id * 4 + branch_id
        for k in range(1, 16):
            other = (my_index + k) % 16
            pl.semaphore_signal(barrier, inc=1, device_id=(data_id, other // 4, other % 4), device_id_type=MESH_ID)
        pl.semaphore_wait(barrier, 15)
        get_lat.wait()
        get_hint.wait()

    mine = pl.ds(pl.multiple_of(side * 64, 64), 64)
    theirs = pl.ds(pl.multiple_of((1 - side) * 64, 64), 64)

    def swap_copy(col, width):
        return remote(msg.at[:, pl.ds(col, width)], u.at[mine, pl.ds(col, width)], us_sem.at[col // 1024], ur_sem.at[col // 1024], partner)

    def emit_hint(col, width, acc):
        base_in = xl[:, pl.ds(col, width)]
        control_in = add_f32(base_in, acc.astype(BF16)).astype(BF16)
        is_base = side == 0
        u[mine, pl.ds(col, width)] = jnp.where(is_base, base_in, control_in)
        msg[:, pl.ds(col, width)] = jnp.where(is_base, control_in, base_in)

    with scope('hint'):
        mm_square(None, 'hint', lambda: hi[...], emit_hint, lambda col, width: swap_copy(col, width).start())
        stream.fill('block')
    def exchange_half(half, first, size, rows):
        ln_rows(u, x, first, size)
        send = remote(x.at[pl.ds(first, size)], x.at[pl.ds(aligned(first + rows, 32), size)], xs_sem.at[half], xr_sem.at[half], peer)
        send.start()
        return send

    def exchange_rows(rows):
        sends = [exchange_half(half, half * (rows // 2), rows // 2, rows) for half in range(2)]
        for send in sends:
            send.wait_recv()
        return sends

    def run_block(is_in, blk, names, bank, fill_in, before_proj):
        rows = 128 if is_in else 64
        chip_rows = 2 * rows
        n_chips, me, combo, owner, extra_dest = layout(is_in)
        extra_slot = 8 // n_chips
        qkv_name, proj_name, up_name, down_name = names

        def chunk(idx, size):
            return pl.ds(aligned(idx * size, size), size)

        def piece_copy(j, dest, slot):
            at = 3 * bank + slot
            return remote(stg.at[j, pl.ds(0, chip_rows)], qin.at[at, chunk(me, chip_rows)], qs_sem.at[j], qr_sem.at[at, me], chip_device(is_in, dest, core))

        def qkv_trip(trip):
            pos = stream.wait(qkv_name, trip, 6)
            for part in range(3):
                both = matmul(x[0:chip_rows, :], columns(pos + 2 * part, 2)).astype(BF16)
                stg[2 * trip, 0:chip_rows, part * LANES:(part + 1) * LANES] = both[:, 0:LANES]
                stg[2 * trip + 1, 0:chip_rows, part * LANES:(part + 1) * LANES] = both[:, LANES:2 * LANES]
            for j in (2 * trip, 2 * trip + 1):
                dest, slot, num, valid = combo(j)

                @pl.when(jnp.logical_and(valid, dest != me))
                def _(j=j, dest=dest, slot=slot):
                    piece_copy(j, dest, slot).start()

                @pl.when(jnp.logical_and(valid, dest == me))
                def _(j=j, slot=slot):
                    qin[3 * bank + slot, chunk(me, chip_rows), :] = stg[j, 0:chip_rows, :]

            stream.used_trip(qkv_name, trip, 5, blk)

        def norm_and_qkv():
            with scope('ln1'):
                sends = exchange_rows(rows)
            with scope('qkv'):
                stream.row(qkv_name, 5)
                pl.loop(0, 5)(qkv_trip)
            for send in sends:
                send.wait_send()

        if is_in:
            pl.when(blk > 0)(norm_and_qkv)
        else:
            norm_and_qkv()
        with scope('fill'):
            fill_in()

        holds = [(extra_dest(0) == me).astype(jnp.int32), jnp.logical_and(extra_dest(1) == me, core == 0).astype(jnp.int32)]
        num_slots = extra_slot + holds[0] + holds[1]

        def slot_pair(slot):
            extra = slot // extra_slot
            return (1 - extra) * (10 * core + slot * n_chips + me) + extra * (10 * core + 8 + holds[1])

        per_chunk = QUERIES // chip_rows

        def query_chunk(i):
            return (me // per_chunk + 1 + i) % (TOK // QUERIES)

        def send_copies(slot, i):
            copies = []
            num = slot_pair(slot)
            first = query_chunk(i) * per_chunk
            chips = [(first + n, True) for n in range(per_chunk)]
            if i == TOK // QUERIES - 1:
                chips = [(me, False)] if per_chunk == 1 else [(me + 1 - 2 * (me % 2), True), (me, False)]
            for n, (idx, other) in enumerate(chips):
                for which in range(2):
                    if not other and which == 0:
                        continue
                    to_core = core if which == 0 else 1 - core
                    src = o_st.at[slot, pl.ds(pl.multiple_of(idx * chip_rows + which * rows, rows), rows)]
                    copies.append(remote(src, a_in.at[pl.ds(0, rows), cols(num * LANES)], as_sem.at[slot, 4 * i + 2 * n + which], ar_sem.at[num], chip_device(is_in, idx, to_core)))
            return copies

        def attend(slot):
            at = 3 * bank + slot
            with scope('att_wait'):
                for k in range(1, n_chips):
                    src = (me + k) % n_chips
                    remote(stg.at[0, pl.ds(0, chip_rows)], qin.at[at, chunk(src, chip_rows)], qs_sem.at[0], qr_sem.at[at, src], peer).wait_recv()
            vt[...] = qin[at, :, 2 * LANES:3 * LANES].T
            low = lax.broadcasted_iota(jnp.int32, (QUERIES, LANES), 1) < 64

            def trip(now, after, top):
                top_next = total = out_a = out_b = None
                if after is not None:
                    q_pair = (qin[at, chunk(query_chunk(after), QUERIES), 0:LANES].astype(F32) * 0.125).astype(BF16)
                    none = jnp.zeros_like(q_pair)
                    q_both = jnp.concatenate([jnp.where(low, q_pair, none), jnp.where(low, none, q_pair)], axis=0)
                for k0 in range(0, TOK, KEYS):
                    keys = slice(k0, k0 + KEYS)
                    if after is not None:
                        score = lax.dot_general(qin[at, keys, LANES:2 * LANES], q_both, (((1,), (1,)), ((), ())), preferred_element_type=F32)
                        sb[after % 2, keys, :] = score
                        part_top = jnp.max(score.reshape(KEYS // 8, 8, 2 * QUERIES), axis=0)
                        top_next = part_top if top_next is None else jnp.maximum(top_next, part_top)
                    if now is not None:
                        weight = jnp.exp(sb[now % 2, keys, :] - top)
                        part_sum = jnp.sum(weight.reshape(KEYS // 8, 8, 2 * QUERIES), axis=0)
                        total = part_sum if total is None else total + part_sum
                        prob = weight.astype(BF16)
                        term_a = matmul(vt[0:64, keys], prob[:, 0:QUERIES])
                        term_b = matmul(vt[64:128, keys], prob[:, QUERIES:2 * QUERIES])
                        out_a = term_a if out_a is None else out_a + term_a
                        out_b = term_b if out_b is None else out_b + term_b
                if now is not None:
                    inv = 1.0 / jnp.sum(total, axis=0, keepdims=True)
                    mixed = jnp.concatenate([out_a * inv[:, 0:QUERIES], out_b * inv[:, QUERIES:2 * QUERIES]], axis=0)
                    o_st[slot, chunk(query_chunk(now), QUERIES), :] = mixed.T.astype(BF16)
                    for copy in send_copies(slot, now):
                        copy.start()
                return None if after is None else jnp.max(top_next, axis=0, keepdims=True)

            last = TOK // QUERIES - 1
            top = trip(None, 0, None)
            for i in range(last):
                top = trip(i, i + 1, top)
            trip(last, None, top)
            a_in[0:rows, cols(slot_pair(slot) * LANES)] = o_st[slot, pl.ds(pl.multiple_of(me * chip_rows, chip_rows), rows), :]

        with scope('att'):
            pl.loop(0, num_slots)(attend)

        with scope('await'):
            @pl.loop(0, 10)
            def _(j):
                dest, slot, num, valid = combo(j)

                @pl.when(jnp.logical_and(valid, dest != me))
                def _():
                    piece_copy(j, dest, slot).wait_send()

            def wait_heads(num):
                plane, dest = owner(num)

                @pl.when(jnp.logical_not(jnp.logical_and(core == plane, me == dest)))
                def _():
                    remote(o_st.at[0, pl.ds(0, rows)], a_in.at[pl.ds(0, rows), cols(num * LANES)], as_sem.at[0, 0], ar_sem.at[num], peer).wait_recv()

            pl.loop(0, 16)(lambda n: wait_heads(n + 2 * (n // 8)))

        main, left = ((0, 1024), (1280, 2304)), ((1024, 1280), (2304, 2432))

        def heads(pick):
            return jnp.concatenate([a_in[0:rows, first:last] for first, last in pick], axis=1)

        def emit_main(col, width, acc):
            po[0:rows, pl.ds(col, width)] = acc

        with scope('proj_main'):
            mm(blk, proj_name, 4, NARROW, lambda: heads(main), emit_main, pick=main)
        with scope('await_left'):
            for num in (8, 9, 18):
                wait_heads(num)
            before_proj()
        with scope('proj'):
            first_unit = stream.places[(proj_name, 0)][0]
            for unit in range(0, 19, 2):
                size = min(2, 19 - unit)
                cut = slice(unit * LANES, (unit + size) * LANES)
                acc = po[0:rows, cut] + matmul(heads(left), columns(first_unit + unit, size, left))
                u[0:rows, cut] = add_f32(u[0:rows, cut], acc.astype(BF16)).astype(BF16)
            for trip in range(5):
                stream.used((proj_name, trip), blk)

            @pl.loop(0, num_slots)
            def _(slot):
                for i in range(TOK // QUERIES):
                    for copy in send_copies(slot, i):
                        copy.wait_send()

        with scope('ln2'):
            sends = exchange_rows(rows)

        def emit_up(col, width, acc):
            hidden = acc.astype(BF16).astype(F32)
            act[0:chip_rows, pl.ds(col, width)] = jax.nn.gelu(hidden).astype(BF16)

        with scope('up'):
            mm_up(blk, up_name, lambda: x[0:chip_rows, :], emit_up)
            for send in sends:
                send.wait_send()

        def partial_copy(col, width):
            tile = col // 512
            return remote(ps.at[pl.ds(0, rows), pl.ds(col, width)], pin.at[pl.ds(0, rows), pl.ds(col, width)], ps_sem.at[tile], pr_sem.at[tile], peer)

        def emit_down(col, width, acc):
            po[0:rows, pl.ds(col, width)] = acc[0:rows]
            ps[0:rows, pl.ds(col, width)] = acc[rows:chip_rows]

        with scope('down'):
            mm_down(blk, down_name, lambda: act[0:chip_rows, :], emit_down, lambda col, width: partial_copy(col, width).start())

        def finish(col, width):
            partial_copy(col, width).wait()
            total = (po[0:rows, pl.ds(col, width)] + pin[0:rows, pl.ds(col, width)]).astype(BF16)
            u[0:rows, pl.ds(col, width)] = add_f32(u[0:rows, pl.ds(col, width)], total).astype(BF16)

        with scope('fin'):
            pl.loop(0, 4)(lambda t: finish(aligned(t * 512, 512), 512))
            finish(4 * 512, 384)

    def make_part(blk, name, idx, after=None, widths=WIDE):
        def emit(col, width, acc):
            part[idx, :, pl.ds(col, width)] = jnp.where(side == 0, u[:, pl.ds(col, width)], acc.astype(BF16))
        mm_square(blk, name, lambda: u[...], emit, after, widths)

    def part_copy(idx):
        return remote(part.at[idx, theirs], rx.at[idx], es_sem.at[idx], er_sem.at[idx], partner)

    def mid_copy(col, width):
        tile = num_in + col // 1024
        return remote(part.at[num_in, theirs, pl.ds(col, width)], rx.at[num_in, :, pl.ds(col, width)], es_sem.at[tile], er_sem.at[tile], partner)

    nothing = lambda: None

    def first_qkv():
        n_chips, me, combo, _, _ = layout(True)

        def piece_copies(j, dest, slot, off):
            return [remote(stg.at[j, pl.ds(pl.multiple_of(off + at, 64), 64)], qin.at[slot, pl.ds(pl.multiple_of(me * 256 + off + at, 64), 64)],
                           qs_sem.at[j], qr_sem.at[slot, me], device(side, dest, core)) for at in (0, 128)]

        stream.row('in_qkv', 5)
        base = stream.places[('in_qkv', 0)][0]

        @pl.loop(0, 2)
        def _(half):
            off = (side + half) % 2 * 64

            @pl.when(half == 1)
            def _():
                each(WIDE, lambda col, width: swap_copy(col, width).wait())

            send = exchange_half(half, pl.multiple_of(off, 64), 64, 128)
            send.wait_recv()
            own, other = pl.ds(pl.multiple_of(off, 64), 64), pl.ds(pl.multiple_of(128 + off, 64), 64)

            @pl.loop(0, 5)
            def _(t):
                pl.when(half == 0)(lambda: (stream.wait('in_qkv', t, 6), None)[1])
                for part in range(3):
                    lhs = jnp.concatenate([x[own, :], x[other, :]], axis=0)
                    both = matmul(lhs, columns(base + 6 * t + 2 * part, 2)).astype(BF16)
                    for odd in range(2):
                        stg[2 * t + odd, own, part * LANES:(part + 1) * LANES] = both[0:64, odd * LANES:(odd + 1) * LANES]
                        stg[2 * t + odd, other, part * LANES:(part + 1) * LANES] = both[64:128, odd * LANES:(odd + 1) * LANES]
                for j in (2 * t, 2 * t + 1):
                    dest, slot, num, valid = combo(j)

                    @pl.when(jnp.logical_and(valid, dest != me))
                    def _(j=j, dest=dest, slot=slot):
                        for copy in piece_copies(j, dest, slot, off):
                            copy.start()

                    @pl.when(jnp.logical_and(valid, dest == me))
                    def _(j=j, slot=slot):
                        for at in (0, 128):
                            qin[slot, pl.ds(pl.multiple_of(me * 256 + off + at, 64), 64), :] = stg[j, pl.ds(pl.multiple_of(off + at, 64), 64), :]
                pl.when(half == 1)(lambda: stream.used_trip('in_qkv', t, 5, 0))

            send.wait_send()

    first_qkv()

    @pl.loop(0, num_blocks)
    def _(blk):
        def send_part():
            pl.when(blk > 0)(lambda: part_copy(blk - 1).start())

        run_block(True, blk, ('in_qkv', 'in_proj', 'in_up', 'in_down'), blk % 2, lambda: make_part(blk, 'in_zero', (blk + num_in) % num_blocks, widths=NARROW), send_part)

    with scope('midpart'):
        make_part(None, 'zero', num_in, lambda col, width: mid_copy(col, width).start())
        for idx in range(num_in):
            part_copy(idx).wait()
            rx[idx] = add_f32(part[idx, mine, :], rx[idx]).astype(BF16)

    def skip_part(blk):
        def emit(col, width, acc):
            skp[:, pl.ds(col, width)] = acc
        mm_square(None, ('skip', blk, 1), lambda: rx[num_in - 1 - blk], emit, widths=NARROW)

    def merge(blk):
        def emit(col, width, acc):
            msg[:, pl.ds(col, width)] = (skp[:, pl.ds(col, width)] + acc).astype(BF16)
        mm_square(None, ('skip', blk, 0), lambda: u[0:64, :], emit)
        u[0:64, :] = msg[...]

    with scope('skip0'):
        skip_part(0)

    def mid_sum(col, width):
        mid_copy(col, width).wait()
        u[0:64, pl.ds(col, width)] = add_f32(part[num_in, mine, pl.ds(col, width)], rx[num_in, :, pl.ds(col, width)]).astype(BF16)

    with scope('midwait'):
        each(WIDE, mid_sum)
    for blk in range(num_out):
        with scope('merge'):
            merge(blk)
        run_block(False, None, (('qkv', blk), ('proj', blk), ('up', blk), ('down', blk)), (num_blocks + blk) % 2, functools.partial(skip_part, blk + 1) if blk + 1 < num_out else nothing, nothing)

    def emit_final(col, width, acc):
        y_ref[0, :, pl.ds(col, width)] = acc.astype(BF16)

    with scope('final'):
        ln_rows(u, x, 0, 64)
        mm_square(None, 'final', lambda: x[0:64, :], emit_final)


def solution(mesh):
    row_spec = P('data', ('seq', 'branch'), None)

    def device_fn(latents, hint_emb, in_qkv, in_proj, in_up, in_down, out_qkv, out_proj, out_up, out_down, hint_proj, zero_proj, skip_proj, final_proj):
        num_in = out_qkv.shape[0]
        in_proj = in_proj.reshape(2, num_in + 1, D, D)
        out_proj = out_proj.reshape(num_in, D, D)
        anywhere = pl.BlockSpec(memory_space=pl.ANY)
        dma = pltpu.SemaphoreType.DMA
        return pl.pallas_call(
            functools.partial(step_kernel, num_in),
            out_shape=jax.ShapeDtypeStruct((1, 64, D), BF16),
            in_specs=[anywhere] * 14,
            out_specs=pl.BlockSpec(memory_space=pltpu.VMEM),
            scratch_shapes=[
                pltpu.VMEM((D, UNITS * LANES), BF16),
                pltpu.VMEM((64, D), BF16),
                pltpu.VMEM((64, D), BF16),
                pltpu.VMEM((64, D), BF16),
                pltpu.VMEM((128, D), BF16),
                pltpu.VMEM((256, D), BF16),
                pltpu.VMEM((256, HALF_UP), BF16),
                pltpu.VMEM((128, D), F32),
                pltpu.VMEM((128, D), F32),
                pltpu.VMEM((128, D), F32),
                pltpu.VMEM((6, TOK, 3 * LANES), BF16),
                pltpu.VMEM((10, 256, 3 * LANES), BF16),
                pltpu.VMEM((3, TOK, LANES), BF16),
                pltpu.VMEM((128, D), BF16),
                pltpu.VMEM((LANES, TOK), BF16),
                pltpu.VMEM((2, TOK, 2 * QUERIES), F32),
                pltpu.VMEM((num_in + 1, 128, D), BF16),
                pltpu.VMEM((num_in + 1, 64, D), BF16),
                pltpu.VMEM((64, D), F32),
                dma((100,)), dma((2,)), dma((2,)), dma((2,)), dma((10,)), dma((10,)),
                dma((10,)), dma((6, 8)), dma((3, 16)), dma((19,)),
                dma((10,)), dma((10,)), dma((num_in + 10,)), dma((num_in + 10,)),
            ],
            compiler_params=pltpu.CompilerParams(collective_id=0, has_side_effects=True, vmem_limit_bytes=67043328),
            name='denoiser_step',
        )(latents, hint_emb, in_qkv, in_proj, in_up, in_down, out_qkv, out_proj, out_up, out_down, hint_proj, zero_proj, skip_proj, final_proj)

    return jax.shard_map(device_fn, mesh=mesh, in_specs=(row_spec, row_spec) + (P(),) * 12, out_specs=row_spec, check_vma=False)
```
